128 devices in a mesh: dp: 8 (over x, y_hi), expert: 16 (over z, y_lo, core).
Axes of the slice: x: 4, y: 4 (y_hi: 2, y_lo: 2; y = y_hi * 2 + y_lo), z: 4, core: 2. Of those that a mesh axis runs over, the one named last changes fastest.
Arguments:
- tokens: bfloat16 [16384, 4096], P(('dp', 'expert')), may hold values from -6 to 6
- cotangent: bfloat16 [16384, 4096], P(('dp', 'expert')), may hold values from -3 to 3
- expert_ids: int32 [16384, 8, 2], P(('dp', 'expert')), may hold values from 0 to 31, as said below
- slot_ids: int32 [16384, 8, 2], P(('dp', 'expert')), may hold values from 0 to 63, as said below
- route_probs: bfloat16 [16384, 8, 2], P(('dp', 'expert')), may hold values from 0.099609375 to 1
- weights_in: bfloat16 [32, 2, 1792, 512], P('expert', None, 'dp'), may hold values from -0.25 to 0.25
- weights_out: bfloat16 [32, 1792, 512], P('expert', 'dp'), may hold values from -0.125 to 0.125
Outputs:
- grad_tokens: bfloat16 [16384, 4096], P(('dp', 'expert'))
- grad_probs: float32 [16384, 8, 2], P(('dp', 'expert'))
- grad_in: bfloat16 [32, 2, 1792, 512], P('expert', None, 'dp')
- grad_out: bfloat16 [32, 1792, 512], P('expert', 'dp')
The draws below stay inside these ranges and needn't reach their ends.
Inputs may be any that keep to these rules, and one draw needn't show every extreme that they name: `expert_ids`: each sub-token names 2 different experts. On each device the experts fall into two sets of 16, and the two ids of a sub-token come one from each set. Every expert is named by exactly 64 sub-tokens of every device. `slot_ids`: for each device and expert, the sub-tokens of that device that name the expert carry distinct slot numbers at the matching position.
All inputs are finite; a program needn't handle non-finite values.
Results may differ from the reference program's by a relative error of at most 0.012.
Values may be sent and summed in bfloat16 or wider, within the bound.
A program may use at most 192 MiB of HBM per device.

```python
import jax
import jax.numpy as jnp
from jax import lax

H = 8
DS = 512
D = 4096
FF = 1792
TOP = 2
EXPERTS = 32
TOK_DEV = 128
TOKENS = 16384
CAP = 64
N_DP = 8
N_EXPERT = 16
DEVICES = 128


def route_plan(key):
    sub_count = TOK_DEV * H
    half_count = EXPERTS // 2
    pool_size = half_count * CAP
    forced = jax.random.randint(jax.random.fold_in(key, 7), (), 0, EXPERTS)
    positions = jnp.arange(pool_size, dtype=jnp.int32)

    def one_device(device_index):
        device_key = jax.random.fold_in(jax.random.fold_in(key, 13), device_index)
        shuffled = jax.random.permutation(jax.random.fold_in(device_key, 1), EXPERTS)
        picked = []
        for which_half in range(2):
            members = shuffled[which_half * half_count:(which_half + 1) * half_count]
            owners = members[positions // CAP]
            scores = jax.random.randint(jax.random.fold_in(device_key, 2 + which_half), (pool_size,), 0, 2 ** 19) * pool_size + positions
            scores = jnp.where(owners == forced, scores - 2 ** 19 * pool_size, scores)
            chosen = jnp.argsort(scores)[:sub_count]
            chosen = chosen[jax.random.permutation(jax.random.fold_in(device_key, 4 + which_half), sub_count)]
            picked.append((owners[chosen], chosen % CAP))
        swapped = jax.random.randint(jax.random.fold_in(device_key, 6), (sub_count,), 0, 2)
        first_expert = jnp.where(swapped == 1, picked[1][0], picked[0][0])
        second_expert = jnp.where(swapped == 1, picked[0][0], picked[1][0])
        first_slot = jnp.where(swapped == 1, picked[1][1], picked[0][1])
        second_slot = jnp.where(swapped == 1, picked[0][1], picked[1][1])
        expert_table = jnp.stack([first_expert, second_expert], axis=1)
        slot_table = jnp.stack([first_slot, second_slot], axis=1)
        return (expert_table, slot_table)
    expert_table, slot_table = jax.vmap(one_device)(jnp.arange(DEVICES, dtype=jnp.int32))
    return (expert_table.reshape(TOKENS, H, TOP).astype(jnp.int32), slot_table.reshape(TOKENS, H, TOP).astype(jnp.int32))


def draw_expert_ids(key, part):
    return route_plan(key)[0]


def draw_slot_ids(key, part):
    return route_plan(key)[1]


def shard_levels(rng, shape, split, low, largest):
    def one(dim, blocks):
        heights = jax.random.uniform(jax.random.fold_in(jax.random.fold_in(rng, 6), dim), (blocks,), jnp.float32, low / len(split), largest / len(split))
        return jnp.repeat(jnp.exp(heights), shape[dim] // blocks).reshape((-1,) + (1,) * (len(shape) - dim - 1))

    factor_of = one(*split[0])
    for cut in split[1:]:
        factor_of = factor_of * one(*cut)
    return factor_of


def gaussian(stream_key, shape, deviation, limit, split=(), kind=jnp.bfloat16):
    gain = shard_levels(stream_key, shape, split, -0.22, 0.18) if split else 1.0
    drawn = jax.random.normal(stream_key, shape, jnp.float32) * deviation * gain
    return jnp.minimum(jnp.maximum(drawn, -limit), limit).astype(kind)


def setup_inputs(seed: int = 0) -> dict:
    arg_keys = jax.random.split(jax.random.key(seed), 8)
    return {
        "tokens": gaussian(arg_keys[0], (TOKENS, D), 1.0, 6.0, ((0, 128),)),
        "cotangent": gaussian(arg_keys[1], (TOKENS, D), 0.5, 3.0, ((0, 128),)),
        "expert_ids": draw_expert_ids(jax.random.fold_in(arg_keys[7], 71), 0),
        "slot_ids": draw_slot_ids(jax.random.fold_in(arg_keys[7], 71), 0),
        "route_probs": jnp.clip(0.099609375 + 0.9003906 * jax.random.uniform(arg_keys[4], (TOKENS, H, TOP), jnp.float32) ** shard_levels(arg_keys[4], (TOKENS, H, TOP), ((0, 128),), -0.2, 0.2), 0.099609375, 1.0).astype(jnp.bfloat16),
        "weights_in": gaussian(arg_keys[5], (EXPERTS, 2, FF, DS), DS ** -0.5, 0.25, ((0, 16), (2, 8))),
        "weights_out": gaussian(arg_keys[6], (EXPERTS, FF, DS), FF ** -0.5, 0.125, ((0, 16), (1, 8))),
    }


def contract_last(former, latter):
    return lax.dot_general(former, latter, (((1,), (1,)), ((), ())), preferred_element_type=jnp.float32)


def expert_backward(inputs, cotangent, weighting, gate_up, down_proj):
    gate_pre = contract_last(inputs, gate_up[0])
    up_pre = contract_last(inputs, gate_up[1])
    sigmoids = jax.nn.sigmoid(gate_pre)
    activated = gate_pre * sigmoids
    hidden = (activated * up_pre).astype(jnp.bfloat16)
    output = jnp.dot(hidden, down_proj, preferred_element_type=jnp.float32)
    router_grad = jnp.sum(output * cotangent.astype(jnp.float32), axis=1).astype(jnp.bfloat16)
    scaled = (weighting.astype(jnp.float32)[:, None] * cotangent.astype(jnp.float32)).astype(jnp.bfloat16)
    dhidden = contract_last(scaled, down_proj)
    gate_grad = (dhidden * up_pre * sigmoids * (1.0 + gate_pre * (1.0 - sigmoids))).astype(jnp.bfloat16)
    up_grad = (dhidden * activated).astype(jnp.bfloat16)
    input_grad = jnp.dot(gate_grad, gate_up[0], preferred_element_type=jnp.float32)
    input_grad = (input_grad + jnp.dot(up_grad, gate_up[1], preferred_element_type=jnp.float32)).astype(jnp.bfloat16)
    return input_grad, router_grad, gate_grad, up_grad, hidden, scaled


def group_sum(left_rows, grouped):
    left_wide = left_rows.reshape(N_DP, N_EXPERT * CAP, left_rows.shape[1]).astype(jnp.float32)
    partial_sums = jnp.einsum("qrf,qrd->qfd", left_wide, grouped, precision=lax.Precision.HIGHEST)
    rounded = lax.optimization_barrier(partial_sums.astype(jnp.bfloat16))
    return jnp.sum(rounded.astype(jnp.float32), axis=0)


def reference(tokens, cotangent, expert_ids, slot_ids, route_probs, weights_in, weights_out):
    sub_count = TOKENS * H
    buffer_rows = EXPERTS * DEVICES * CAP
    device_of = (jnp.arange(sub_count, dtype=jnp.int32) // (TOK_DEV * H)).astype(jnp.int32)
    placed = expert_ids.reshape(sub_count, TOP).astype(jnp.int32) * (DEVICES * CAP) + device_of[:, None] * CAP + slot_ids.reshape(sub_count, TOP).astype(jnp.int32)
    flat_place = placed.reshape(-1).astype(jnp.int32)

    def spread(values):
        doubled = jnp.broadcast_to(values[:, None, :], (sub_count, TOP, DS)).reshape(sub_count * TOP, DS)
        filled = jnp.zeros((buffer_rows, DS), values.dtype).at[flat_place].set(doubled)
        return filled.reshape(EXPERTS, DEVICES * CAP, DS)

    input_buffer = spread(tokens.reshape(sub_count, DS))
    cotangent_buffer = spread(cotangent.reshape(sub_count, DS))
    prob_buffer = jnp.zeros((buffer_rows,), route_probs.dtype).at[flat_place].set(route_probs.reshape(-1))
    prob_buffer = prob_buffer.reshape(EXPERTS, DEVICES * CAP)

    def one_expert(packed):
        rows_in, rows_cot, rows_prob, gate_up, down_proj = packed
        input_grad, router_grad, gate_grad, up_grad, hidden, scaled = expert_backward(rows_in, rows_cot, rows_prob, gate_up, down_proj)
        grouped = rows_in.reshape(N_DP, N_EXPERT * CAP, DS).astype(jnp.float32)
        gate_sum = group_sum(gate_grad, grouped)
        up_sum = group_sum(up_grad, grouped)
        down_sum = group_sum(hidden, scaled.reshape(N_DP, N_EXPERT * CAP, DS).astype(jnp.float32))
        pair_sum = jnp.stack([gate_sum, up_sum]).astype(jnp.bfloat16)
        return input_grad, router_grad, pair_sum, down_sum.astype(jnp.bfloat16)

    input_grads, router_grads, grad_in, grad_out = lax.map(one_expert, (input_buffer, cotangent_buffer, prob_buffer, weights_in, weights_out))
    back_rows = input_grads.reshape(buffer_rows, DS)[flat_place].reshape(sub_count, TOP, DS).astype(jnp.float32)
    grad_tokens = jnp.sum(back_rows, axis=1).astype(jnp.bfloat16).reshape(TOKENS, D)
    grad_probs = router_grads.reshape(buffer_rows)[flat_place].reshape(TOKENS, H, TOP).astype(jnp.float32)
    return grad_tokens, grad_probs, grad_in, grad_out
```

```python
import functools

import jax
import jax.numpy as jnp
from jax import lax
from jax.experimental import pallas as pl
from jax.experimental.pallas import tpu as pltpu
from jax.sharding import PartitionSpec as P

H = 8
NX = 4
NH = 2
MESH = pl.DeviceIdType.MESH
F32 = jnp.float32
BF16 = jnp.bfloat16
GROUP = 4
JB = 256


def dot_nn(a, b):
    return lax.dot_general(a, b, (((1,), (0,)), ((), ())), preferred_element_type=F32)


def dot_nt(a, b):
    return lax.dot_general(a, b, (((1,), (1,)), ((), ())), preferred_element_type=F32)


def dot_tn(a, b):
    return lax.dot_general(a, b, (((0,), (0,)), ((), ())), preferred_element_type=F32)


def kernel(
    dims,
    tok,
    cot,
    place_row,
    prob_row,
    place_col,
    w_in,
    w_out,
    gtok,
    gprob,
    gin,
    gout,
    tok_rows,
    cot_rows,
    x_send,
    s_send,
    x_all,
    s_all,
    wall,
    acts,
    dxt,
    racc,
    part,
    rs_far,
    rs_sum,
    rs_dir,
    stage,
    swap,
    dx_send,
    back,
    r_send,
    r_back,
    gacc,
    w_ssem,
    w_rsem,
    x_ssem,
    x_rsem,
    s_ssem,
    s_rsem,
    g_ssem,
    g_rsem,
    d_ssem,
    d_rsem,
    r_ssem,
    r_rsem,
):
    ng, toks, d, fs, cap = dims
    experts = NH * ng
    peers = NH * ng
    rows = toks * H
    slots = peers * cap
    half = fs // 2
    fc = NH * fs

    dp = lax.axis_index("dp")
    g = lax.axis_index("expert")
    x = dp // NH
    h = dp % NH
    right = (x + 1) % NX
    left = (x + 3) % NX
    far = (x + 2) % NX
    other = 1 - h
    my_e = g * NH + h
    my_b = h * ng + g

    def remote(src, dst, ssem, rsem, to_dp, to_g):
        return pltpu.make_async_remote_copy(
            src_ref=src,
            dst_ref=dst,
            send_sem=ssem,
            recv_sem=rsem,
            device_id=(to_dp, to_g),
            device_id_type=MESH,
        )

    barrier = pltpu.get_barrier_semaphore()

    def greet(t, carry):
        u = (my_b + t) % peers
        pl.semaphore_signal(
            barrier, inc=1, device_id=(x * NH + u // ng, u % ng), device_id_type=MESH
        )
        return carry

    lax.fori_loop(1, peers, greet, 0)
    for nx in (right, left):
        pl.semaphore_signal(barrier, inc=1, device_id=(nx * NH + h, g), device_id_type=MESH)
    pl.semaphore_wait(barrier, peers + 1)

    to_right = (right * NH + h, g)
    to_left = (left * NH + h, g)
    to_partner = (x * NH + other, g)

    def wcopy(k, src, dst, to):
        return remote(src, dst, w_ssem.at[k], w_rsem.at[k], *to)

    first = [
        wcopy(0, w_in.at[other], wall.at[x, pl.ds(0, 2), h], to_partner),
        wcopy(1, w_out.at[other], wall.at[x, 2, h], to_partner),
        wcopy(2, w_in.at[h], wall.at[x, pl.ds(0, 2), h], to_right),
        wcopy(3, w_out.at[h], wall.at[x, 2, h], to_right),
        wcopy(4, w_in.at[h], wall.at[x, pl.ds(0, 2), h], to_left),
        wcopy(5, w_out.at[h], wall.at[x, 2, h], to_left),
    ]
    for c in first:
        c.start()

    for n in range(H):
        tok_rows[n * toks : (n + 1) * toks, :] = tok[:, n * d : (n + 1) * d]
        cot_rows[n * toks : (n + 1) * toks, :] = cot[:, n * d : (n + 1) * d]

    groups = experts // GROUP
    span = GROUP * cap

    def send_expert(e):
        to = (x * NH + e % NH, e // NH)

        @pl.when(e != my_e)
        def _():
            remote(x_send.at[e], x_all.at[my_b], x_ssem.at[e], x_rsem.at[my_b], *to).start()
            remote(s_send.at[e], s_all.at[my_b], s_ssem.at[e], s_rsem.at[my_b], *to).start()

    def dispatch(i, carry):
        gb = (my_e // GROUP + i) % groups
        ids = lax.broadcasted_iota(jnp.int32, (span, rows), 0) + gb * span
        hit0 = place_row[0:1, :] == ids
        hit1 = place_row[1:2, :] == ids
        one = jnp.where(hit0 | hit1, 1.0, 0.0).astype(BF16)
        wgt = jnp.where(hit0, prob_row[0:1, :], jnp.where(hit1, prob_row[1:2, :], 0.0)).astype(BF16)
        x_send[pl.ds(gb * GROUP, GROUP)] = (
            dot_nn(one, tok_rows[...]).astype(BF16).reshape(GROUP, cap, d)
        )
        s_send[pl.ds(gb * GROUP, GROUP)] = (
            dot_nn(wgt, cot_rows[...]).astype(BF16).reshape(GROUP, cap, d)
        )
        for j in range(GROUP):
            send_expert(gb * GROUP + j)
        return carry

    lax.fori_loop(0, groups, dispatch, 0)
    wall[x, 0:2, h] = w_in[h]
    wall[x, 2, h] = w_out[h]
    x_all[my_b] = x_send[my_e]
    s_all[my_b] = s_send[my_e]

    def wforward(k, slot, part_rows, plane, to):
        ref = wall.at[slot, pl.ds(0, 3), plane, part_rows]
        return wcopy(k, ref, ref, to)

    top, bottom, full = pl.ds(0, half), pl.ds(half, half), pl.ds(0, fs)
    first[2].wait_recv()
    first[3].wait_recv()
    f6 = wforward(6, left, top, h, to_right)
    f6.start()
    first[4].wait_recv()
    first[5].wait_recv()
    f7 = wforward(7, right, bottom, h, to_left)
    f7.start()
    first[0].wait_recv()
    first[1].wait_recv()
    f8 = wforward(8, x, full, other, to_right)
    f8.start()
    f9 = wforward(9, x, full, other, to_left)
    f9.start()
    f8.wait_recv()
    f10 = wforward(10, left, top, other, to_right)
    f10.start()
    f9.wait_recv()
    f11 = wforward(11, right, bottom, other, to_left)
    f11.start()

    def arrived(t, carry):
        b = (my_b + t) % peers
        remote(x_send.at[0], x_all.at[b], x_ssem.at[0], x_rsem.at[b], x * NH, g).wait_recv()
        remote(s_send.at[0], s_all.at[b], s_ssem.at[0], s_rsem.at[b], x * NH, g).wait_recv()
        return carry

    lax.fori_loop(1, peers, arrived, 0)
    for c in (f6, f7, f10, f11):
        c.wait_recv()

    racc[...] = jnp.zeros_like(racc)
    dxt[...] = jnp.zeros_like(dxt)

    def chunk(s, carry):
        off = jnp.where(s == 0, 2, jnp.where(s == 1, 1, jnp.where(s == 2, 3, 0)))
        xc = (x + off) % NX

        def block(j, c2):
            at = pl.ds(pl.multiple_of(j * JB, JB), JB)
            some = pl.ds(j * (JB // cap), JB // cap)
            xb = x_all[some].reshape(JB, d)
            sb = s_all[some].reshape(JB, d)
            wg = wall[xc, 0].reshape(fc, d)
            wu = wall[xc, 1].reshape(fc, d)
            wo = wall[xc, 2].reshape(fc, d)
            gate = dot_nt(wg, xb)
            up = dot_nt(wu, xb)
            dh = dot_nt(wo, sb)
            sg = 0.5 * jnp.tanh(0.5 * gate) + 0.5
            a = gate * sg
            du = dh * a
            dg = dh * up * (sg + a * (1.0 - sg))
            hid = a * up
            dgb = dg.astype(BF16)
            dub = du.astype(BF16)
            acts[0, :, at] = dgb
            acts[1, :, at] = dub
            acts[2, :, at] = hid.astype(BF16)
            racc[:, at] += jnp.sum((du * up).reshape(fc // 8, 8, JB), axis=0)
            dxt[:, at] += dot_tn(wg, dgb) + dot_tn(wu, dub)
            return c2

        lax.fori_loop(0, slots // JB, block, 0)
        xa = x_all[...].reshape(slots, d)
        sa = s_all[...].reshape(slots, d)
        part[s, 0] = dot_nn(acts[0], xa).astype(BF16).reshape(NH, fs, d)
        part[s, 1] = dot_nn(acts[1], xa).astype(BF16).reshape(NH, fs, d)
        part[s, 2] = dot_nn(acts[2], sa).astype(BF16).reshape(NH, fs, d)

        @pl.when(s == 0)
        def _():
            far_right.start()
            far_left.start()

        @pl.when(s == 1)
        def _():
            dir_right.start()

        @pl.when(s == 2)
        def _():
            dir_left.start()
            far_right.wait_recv()
            add_far(0, 1, top)
            sum_right.start()
            far_left.wait_recv()
            add_far(1, 2, bottom)
            sum_left.start()

        return carry

    def gcopy(k, src, dst, to):
        return remote(src, dst, g_ssem.at[k], g_rsem.at[k], *to)

    def piece(s, part_rows):
        return part.at[s, pl.ds(0, 3), pl.ds(0, NH), part_rows]

    far_right = gcopy(0, piece(0, top), rs_far.at[0], to_right)
    far_left = gcopy(1, piece(0, bottom), rs_far.at[1], to_left)
    dir_right = gcopy(2, piece(1, bottom), rs_dir.at[0], to_right)
    dir_left = gcopy(3, piece(2, top), rs_dir.at[1], to_left)
    sum_right = gcopy(4, stage.at[0], rs_sum.at[0], to_right)
    sum_left = gcopy(5, stage.at[1], rs_sum.at[1], to_left)

    def add_far(side, s, part_rows):
        for m in range(3):
            stage[side, m] = (
                rs_far[side, m].astype(F32) + part[s, m, :, part_rows, :].astype(F32)
            ).astype(BF16)

    lax.fori_loop(0, NX, chunk, 0)

    def turn(i, carry):
        at = pl.ds(pl.multiple_of(i * 256, 256), 256)
        dx_send[pl.ds(i * (256 // cap), 256 // cap)] = (
            jnp.transpose(dxt[:, at], (1, 0)).astype(BF16).reshape(256 // cap, cap, d)
        )
        return carry

    lax.fori_loop(0, slots // 256, turn, 0)
    r_row = jnp.sum(racc[...], axis=0, keepdims=True)
    for i in range(slots // 128):
        r_send[i] = jnp.broadcast_to(r_row[:, i * 128 : (i + 1) * 128], (8, 128))

    def give(t, carry):
        b = (my_b + t) % peers
        to = (x * NH + b // ng, b % ng)
        remote(dx_send.at[b], back.at[my_e], d_ssem.at[b], d_rsem.at[my_e], *to).start()
        remote(
            r_send.at[b * cap // 128], r_back.at[my_e], r_ssem.at[b], r_rsem.at[my_e], *to
        ).start()
        return carry

    lax.fori_loop(1, peers, give, 0)
    back[my_e] = dx_send[my_b]
    r_back[my_e] = r_send[my_b * cap // 128]

    far_from = [(dir_right, sum_right), (dir_left, sum_left)]
    for pair in far_from:
        for c in pair:
            c.wait_recv()

    def total(m, plane, lower):
        mine = part[3, m, plane, pl.ds(half if lower else 0, half), :].astype(F32)
        if lower:
            got = rs_dir[0, m, plane].astype(F32) + rs_sum[1, m, plane].astype(F32)
        else:
            got = rs_dir[1, m, plane].astype(F32) + rs_sum[0, m, plane].astype(F32)
        return (mine + got).astype(BF16)

    for m in range(3):
        swap[m, 0:half] = total(m, other, False)
        swap[m, half:fs] = total(m, other, True)
    swap_in = gcopy(6, swap.at[pl.ds(0, 2)], gin.at[h], to_partner)
    swap_out = gcopy(7, swap.at[2], gout.at[h], to_partner)
    swap_in.start()
    swap_out.start()
    for m in range(2):
        gin[h, m, 0:half] = total(m, h, False)
        gin[h, m, half:fs] = total(m, h, True)
    gout[h, 0:half] = total(2, h, False)
    gout[h, half:fs] = total(2, h, True)

    def gather_back(t, carry):
        b = (my_b + t) % peers
        e = (b % ng) * NH + b // ng
        remote(dx_send.at[0], back.at[e], d_ssem.at[0], d_rsem.at[e], x * NH, g).wait_recv()
        remote(r_send.at[0], r_back.at[e], r_ssem.at[0], r_rsem.at[e], x * NH, g).wait_recv()
        return carry

    lax.fori_loop(1, peers, gather_back, 0)

    def combine(n, carry):
        at = pl.ds(pl.multiple_of(n * toks, toks), toks)
        pc = place_col[at, :]
        ids = lax.broadcasted_iota(jnp.int32, (toks, slots), 1)
        one = jnp.where((pc[:, 0:1] == ids) | (pc[:, 1:2] == ids), 1.0, 0.0).astype(BF16)
        gacc[at, :] = dot_nn(one, back[...].reshape(slots, d))
        return carry

    lax.fori_loop(0, H, combine, 0)
    for n in range(H):
        gtok[:, n * d : (n + 1) * d] = gacc[n * toks : (n + 1) * toks, :].astype(BF16)

    r_mine = r_back[:, 0, :]
    shift = (my_b % (128 // cap)) * cap
    for k in range(2):
        pr = place_row[k : k + 1, :]
        expert = lax.shift_right_logical(pr, cap.bit_length() - 1)
        slot = lax.bitwise_and(pr, cap - 1)
        pick = jnp.where(
            lax.broadcasted_iota(jnp.int32, (experts, rows), 0) == expert, 1.0, 0.0
        )
        table = lax.dot_general(
            r_mine,
            pick,
            (((0,), (0,)), ((), ())),
            precision=lax.Precision.HIGHEST,
            preferred_element_type=F32,
        )
        lanes = lax.broadcasted_iota(jnp.int32, (128, rows), 0)
        value = jnp.sum(jnp.where(lanes == slot + shift, table, 0.0), axis=0, keepdims=True)
        gprob[k : k + 1, :] = value / prob_row[k : k + 1, :]

    for c in first + [f6, f7, f8, f9, f10, f11]:
        c.wait_send()
    for c in (far_right, far_left, dir_right, dir_left, sum_right, sum_left):
        c.wait_send()
    swap_in.wait()
    swap_out.wait()

    def drain(t, carry):
        b = (my_b + t) % peers
        e = (b % ng) * NH + b // ng
        remote(x_send.at[0], x_all.at[0], x_ssem.at[e], x_rsem.at[0], x * NH, g).wait_send()
        remote(s_send.at[0], s_all.at[0], s_ssem.at[e], s_rsem.at[0], x * NH, g).wait_send()
        remote(dx_send.at[0], back.at[0], d_ssem.at[b], d_rsem.at[0], x * NH, g).wait_send()
        remote(r_send.at[0], r_back.at[0], r_ssem.at[b], r_rsem.at[0], x * NH, g).wait_send()
        return carry

    lax.fori_loop(1, peers, drain, 0)


def body(tokens, cotangent, expert_ids, slot_ids, route_probs, weights_in, weights_out):
    ng = lax.axis_size("expert")
    toks = tokens.shape[0]
    d = tokens.shape[1] // H
    fs = weights_in.shape[2]
    experts = NH * ng
    peers = experts
    rows = toks * H
    cap = rows * 2 // experts
    slots = peers * cap
    half = fs // 2
    fc = NH * fs

    place = jnp.transpose(expert_ids * cap + slot_ids, (2, 1, 0)).reshape(2, rows)
    probs = jnp.transpose(route_probs, (2, 1, 0)).reshape(2, rows).astype(F32)
    place_col = jnp.transpose(place, (1, 0))

    vmem = pl.BlockSpec(memory_space=pltpu.VMEM)
    dma = pltpu.SemaphoreType.DMA
    gtok, gprob, gin, gout = pl.pallas_call(
        functools.partial(kernel, (ng, toks, d, fs, cap)),
        out_shape=(
            jax.ShapeDtypeStruct((toks, H * d), BF16),
            jax.ShapeDtypeStruct((2, rows), F32),
            jax.ShapeDtypeStruct((2, 2, fs, d), BF16),
            jax.ShapeDtypeStruct((2, fs, d), BF16),
        ),
        in_specs=[vmem] * 7,
        out_specs=(vmem,) * 4,
        scratch_shapes=[
            pltpu.VMEM((rows, d), BF16),
            pltpu.VMEM((rows, d), BF16),
            pltpu.VMEM((experts, cap, d), BF16),
            pltpu.VMEM((experts, cap, d), BF16),
            pltpu.VMEM((peers, cap, d), BF16),
            pltpu.VMEM((peers, cap, d), BF16),
            pltpu.VMEM((NX, 3, NH, fs, d), BF16),
            pltpu.VMEM((3, fc, slots), BF16),
            pltpu.VMEM((d, slots), F32),
            pltpu.VMEM((8, slots), F32),
            pltpu.VMEM((NX, 3, NH, fs, d), BF16),
            pltpu.VMEM((2, 3, NH, half, d), BF16),
            pltpu.VMEM((2, 3, NH, half, d), BF16),
            pltpu.VMEM((2, 3, NH, half, d), BF16),
            pltpu.VMEM((2, 3, NH, half, d), BF16),
            pltpu.VMEM((3, fs, d), BF16),
            pltpu.VMEM((peers, cap, d), BF16),
            pltpu.VMEM((experts, cap, d), BF16),
            pltpu.VMEM((slots // 128, 8, 128), F32),
            pltpu.VMEM((experts, 8, 128), F32),
            pltpu.VMEM((rows, d), F32),
            dma((12,)),
            dma((12,)),
            dma((experts,)),
            dma((peers,)),
            dma((experts,)),
            dma((peers,)),
            dma((8,)),
            dma((8,)),
            dma((peers,)),
            dma((experts,)),
            dma((peers,)),
            dma((experts,)),
        ],
        compiler_params=pltpu.CompilerParams(
            collective_id=0, has_side_effects=True, vmem_limit_bytes=66_000_000
        ),
        name="moe_backward",
    )(tokens, cotangent, place, probs, place_col, weights_in, weights_out)
    grad_probs = jnp.transpose(gprob.reshape(2, H, toks), (2, 1, 0))
    return gtok, grad_probs, gin, gout


def solution(mesh):
    return jax.shard_map(
        body,
        mesh=mesh,
        in_specs=(
            P(("dp", "expert"), None),
            P(("dp", "expert"), None),
            P(("dp", "expert"), None, None),
            P(("dp", "expert"), None, None),
            P(("dp", "expert"), None, None),
            P("expert", None, "dp", None),
            P("expert", "dp", None),
        ),
        out_specs=(
            P(("dp", "expert"), None),
            P(("dp", "expert"), None, None),
            P("expert", None, "dp", None),
            P("expert", "dp", None),
        ),
        check_vma=False,
    )
```

```python
import functools

import jax
import jax.numpy as jnp
from jax import lax
from jax.experimental import pallas as pl
from jax.experimental.pallas import tpu as pltpu
from jax.sharding import PartitionSpec as P

H = 8
NX = 4
NH = 2
MESH = pl.DeviceIdType.MESH
F32 = jnp.float32
BF16 = jnp.bfloat16
BLOCKS = 4
FLIP = True
GRID = {16: (4, 2, 2), 2: (1, 1, 2)}


def dot_nn(a, b):
    return lax.dot_general(a, b, (((1,), (0,)), ((), ())), preferred_element_type=F32)


def dot_nt(a, b):
    return lax.dot_general(a, b, (((1,), (1,)), ((), ())), preferred_element_type=F32)


def dot_tn(a, b):
    return lax.dot_general(a, b, (((0,), (0,)), ((), ())), preferred_element_type=F32)


def send_order(nz, ny, nc):
    order = []
    for dc in range(nc):
        for s in range(nz):
            for dy in range(ny):
                order.append((dy, (3 * dy + s) % nz, dc))
    return order


def kernel(
    dims,
    tok,
    cot,
    place_row,
    prob_row,
    place_col,
    w_in,
    w_out,
    gtok,
    gprob,
    gin,
    gout,
    rows_buf,
    xs_send,
    xs_all,
    wall,
    acts,
    dx,
    racc,
    rs_far,
    rs_sum,
    rs_dir,
    back,
    r_send,
    r_back,
    w_ssem,
    w_rsem,
    x_ssem,
    x_rsem,
    g_ssem,
    g_rsem,
    d_ssem,
    d_rsem,
    r_ssem,
    r_rsem,
):
    ng, toks, d, fs, cap = dims
    nz, nyl, nc = GRID[ng]
    ny = NH * nyl
    peers = NH * ng
    rows = toks * H
    slots = peers * cap
    half = fs // 2
    fc = NH * fs
    jb = slots // BLOCKS
    per = peers // BLOCKS
    order = send_order(nz, ny, nc)

    dp = lax.axis_index("dp")
    g = lax.axis_index("expert")
    x = dp // NH
    h = dp % NH
    core = g % nc
    y = h * nyl + (g // nc) % nyl
    z = g // (nc * nyl)
    right = (x + 1) % NX
    left = (x + 3) % NX
    far = (x + 2) % NX
    other = 1 - h
    me = g * NH + h

    def place_of(ty, tz, tc):
        return ((tz * nyl + ty % nyl) * nc + tc) * NH + ty // nyl

    def target(t):
        dy, dz, dc = order[t]
        sign = 1 - 2 * core if FLIP else 1
        return place_of(
            (y + sign * dy + ny) % ny, (z + sign * dz + nz) % nz, (core + dc) % nc
        )

    def source(t):
        dy, dz, dc = order[t]
        tc = (core + dc) % nc
        sign = 1 - 2 * tc if FLIP else 1
        return place_of((y - sign * dy + ny) % ny, (z - sign * dz + nz) % nz, tc)

    def device(u):
        return (x * NH + u % NH, u // NH)

    def remote(src, dst, ssem, rsem, to):
        return pltpu.make_async_remote_copy(
            src_ref=src,
            dst_ref=dst,
            send_sem=ssem,
            recv_sem=rsem,
            device_id=to,
            device_id_type=MESH,
        )

    barrier = pltpu.get_barrier_semaphore()
    to_right = (right * NH + h, g)
    to_left = (left * NH + h, g)
    to_partner = (x * NH + other, g)
    for t in range(1, peers):
        pl.semaphore_signal(barrier, inc=1, device_id=device(target(t)), device_id_type=MESH)
    for to in (to_right, to_left):
        pl.semaphore_signal(barrier, inc=1, device_id=to, device_id_type=MESH)

    for n in range(H):
        rows_buf[n * toks : (n + 1) * toks, :] = tok[:, n * d : (n + 1) * d]
        rows_buf[rows + n * toks : rows + (n + 1) * toks, :] = cot[:, n * d : (n + 1) * d]
    pl.semaphore_wait(barrier, peers + 1)

    def wcopy(k, src, dst, to):
        return remote(src, dst, w_ssem.at[k], w_rsem.at[k], to)

    first = [
        wcopy(0, w_in.at[other], wall.at[x, pl.ds(0, 2), h], to_partner),
        wcopy(1, w_out.at[other], wall.at[x, 2, h], to_partner),
        wcopy(2, w_in.at[h], wall.at[x, pl.ds(0, 2), h], to_right),
        wcopy(3, w_out.at[h], wall.at[x, 2, h], to_right),
        wcopy(4, w_in.at[h], wall.at[x, pl.ds(0, 2), h], to_left),
        wcopy(5, w_out.at[h], wall.at[x, 2, h], to_left),
    ]
    for c in first:
        c.start()

    pairs = nz * nyl
    width = min(2, pairs)
    span = NH * cap

    def xs_copy(t):
        u = target(t)
        return remote(xs_send.at[u], xs_all.at[t], x_ssem.at[t], x_rsem.at[t], device(u))

    for dc in range(nc):
        cc = (core + dc) % nc

        def dispatch(i, carry):
            row = lax.broadcasted_iota(jnp.int32, (width * span, rows), 0)
            ids = row + ((i * width * nc + cc) * span)
            if width == 2:
                ids = ids + jnp.where(row >= span, (nc - 1) * span, 0)
            hit0 = place_row[0:1, :] == ids
            hit1 = place_row[1:2, :] == ids
            one = jnp.where(hit0 | hit1, 1.0, 0.0).astype(BF16)
            wgt = jnp.where(hit0, prob_row[0:1, :], jnp.where(hit1, prob_row[1:2, :], 0.0))
            xr = dot_nn(one, rows_buf[0:rows, :]).astype(BF16)
            sr = dot_nn(wgt.astype(BF16), rows_buf[rows : 2 * rows, :]).astype(BF16)
            for j in range(width):
                e0 = ((i * width + j) * nc + cc) * NH
                for k in range(NH):
                    at = (j * NH + k) * cap
                    xs_send[e0 + k, 0] = xr[at : at + cap, :]
                    xs_send[e0 + k, 1] = sr[at : at + cap, :]
            return carry

        lax.fori_loop(0, pairs // width, dispatch, 0)
        for t in range(1, peers):
            if order[t][2] == dc:
                xs_copy(t).start()

    wall[x, 0:2, h] = w_in[h]
    wall[x, 2, h] = w_out[h]
    xs_all[0] = xs_send[me]
    racc[...] = jnp.zeros_like(racc)
    dx[...] = jnp.zeros_like(dx)

    def wforward(k, slot, part_rows, plane, to):
        ref = wall.at[slot, pl.ds(0, 3), plane, part_rows]
        return wcopy(k, ref, ref, to)

    top, bottom, full = pl.ds(0, half), pl.ds(half, half), pl.ds(0, fs)

    def xs_wait(i):
        for t in range(max(1, i * per), (i + 1) * per):
            xs_copy(t).wait_recv()

    def block(xc, i):
        at = pl.ds(pl.multiple_of(i * jb, jb), jb)
        some = pl.ds(i * per, per)
        xb = xs_all[some, 0].reshape(jb, d)
        sb = xs_all[some, 1].reshape(jb, d)
        wg = wall[xc, 0].reshape(fc, d)
        wu = wall[xc, 1].reshape(fc, d)
        wo = wall[xc, 2].reshape(fc, d)
        gate = dot_nt(wg, xb)
        up = dot_nt(wu, xb)
        dh = dot_nt(wo, sb)
        sg = 0.5 * jnp.tanh(0.5 * gate) + 0.5
        a = gate * sg
        du = dh * a
        dg = dh * up * (sg + a * (1.0 - sg))
        dgb = dg.astype(BF16)
        dub = du.astype(BF16)
        acts[xc, 0, :, :, at] = dgb.reshape(NH, fs, jb)
        acts[xc, 1, :, :, at] = dub.reshape(NH, fs, jb)
        acts[xc, 2, :, :, at] = (a * up).astype(BF16).reshape(NH, fs, jb)
        racc[:, at] += jnp.sum((du * up).reshape(fc // 8, 8, jb), axis=0)
        dx[at, :] += dot_tn(dgb, wg) + dot_tn(dub, wu)

    def sweep(count, xc_of, i_of):
        def step(n, carry):
            block(xc_of(n), i_of(n))
            return carry

        lax.fori_loop(0, count, step, 0)

    first[2].wait_recv()
    first[3].wait_recv()
    f6 = wforward(6, left, top, h, to_right)
    f6.start()
    first[4].wait_recv()
    first[5].wait_recv()
    f7 = wforward(7, right, bottom, h, to_left)
    f7.start()
    first[0].wait_recv()
    first[1].wait_recv()
    f8 = wforward(8, x, full, other, to_right)
    f8.start()
    f9 = wforward(9, x, full, other, to_left)
    f9.start()
    xs_wait(0)
    sweep(1, lambda n: x, lambda n: n * 0)
    f8.wait_recv()
    f10 = wforward(10, left, top, other, to_right)
    f10.start()
    f9.wait_recv()
    f11 = wforward(11, right, bottom, other, to_left)
    f11.start()
    sweep(2, lambda n: (x + 1 + 2 * n) % NX, lambda n: n * 0)
    xs_wait(1)
    sweep(3, lambda n: (x + jnp.where(n == 2, 3, n)) % NX, lambda n: n * 0 + 1)
    for c in (f6, f7, f10, f11):
        c.wait_recv()
    sweep(2, lambda n: far, lambda n: n)
    xs_wait(2)
    sweep(4, lambda n: (x + 2 + n) % NX, lambda n: n * 0 + 2)
    xs_wait(3)

    def give(i):
        for k in range(per):
            t = i * per + k
            dst = rows_buf.at[pl.ds(t * cap, cap)]
            if t:
                u = source(t)
                remote(dst, back.at[me], d_ssem.at[t], d_rsem.at[me], device(u)).start()
                remote(r_send.at[t], r_back.at[me], r_ssem.at[t], r_rsem.at[me], device(u)).start()
            else:
                back[me] = rows_buf[0:cap, :]
                r_back[me] = r_send[0]

    def finish(i):
        rows_buf[i * jb : (i + 1) * jb, :] = dx[i * jb : (i + 1) * jb, :].astype(BF16)
        r_row = jnp.sum(racc[:, i * jb : (i + 1) * jb], axis=0, keepdims=True)
        for k in range(per):
            v = r_row[:, k * cap : (k + 1) * cap]
            r_send[i * per + k] = jnp.broadcast_to(jnp.concatenate([v, v], axis=1), (8, 128))

    planes = (other, h)

    def gcopy(k, src, dst, to):
        return remote(src, dst, g_ssem.at[k], g_rsem.at[k], to)

    def piece(xc, part_rows, plane):
        return acts.at[xc, pl.ds(0, 3), plane, part_rows, pl.ds(0, d)]

    far_right = [gcopy(p, piece(far, top, planes[p]), rs_far.at[0, p], to_right) for p in (0, 1)]
    far_left = [
        gcopy(2 + p, piece(far, bottom, planes[p]), rs_far.at[1, p], to_left) for p in (0, 1)
    ]
    dir_right = [
        gcopy(4 + p, piece(right, bottom, planes[p]), rs_dir.at[0, p], to_right) for p in (0, 1)
    ]
    dir_left = [
        gcopy(6 + p, piece(left, top, planes[p]), rs_dir.at[1, p], to_left) for p in (0, 1)
    ]
    sum_right = [
        gcopy(8 + p, piece(right, top, planes[p]), rs_sum.at[0, p], to_right) for p in (0, 1)
    ]
    sum_left = [
        gcopy(10 + p, piece(left, bottom, planes[p]), rs_sum.at[1, p], to_left) for p in (0, 1)
    ]

    def weight_grads(xc):
        xa = xs_all[:, 0].reshape(slots, d)
        sa = xs_all[:, 1].reshape(slots, d)
        for m, against in ((0, xa), (1, xa), (2, sa)):
            grad = dot_nn(acts[xc, m].reshape(fc, slots), against)
            acts[xc, m, :, :, 0:d] = grad.astype(BF16).reshape(NH, fs, d)

    def add_far(side, p):
        xc, part_rows = (right, top) if side == 0 else (left, bottom)
        for m in range(3):
            mine = acts[xc, m, planes[p], part_rows, 0:d].astype(F32)
            acts[xc, m, planes[p], part_rows, 0:d] = (
                rs_far[side, p, m].astype(F32) + mine
            ).astype(BF16)

    def last(n, carry):
        xc = (x + jnp.where(n == 0, 2, jnp.where(n == 1, 1, jnp.where(n == 2, 3, 0)))) % NX
        block(xc, BLOCKS - 1)

        @pl.when(n == 3)
        def _():
            finish(3)
            give(3)

        weight_grads(xc)

        @pl.when(n == 0)
        def _():
            for p in (0, 1):
                far_right[p].start()
                far_left[p].start()
            for i in range(3):
                finish(i)
                give(i)

        @pl.when(n == 1)
        def _():
            dir_right[0].start()

        @pl.when(n == 2)
        def _():
            dir_left[0].start()
            far_right[0].wait_recv()
            add_far(0, 0)
            sum_right[0].start()
            dir_right[1].start()
            far_left[0].wait_recv()
            add_far(1, 0)
            sum_left[0].start()
            dir_left[1].start()

        return carry

    lax.fori_loop(0, NX, last, 0)
    far_right[1].wait_recv()
    add_far(0, 1)
    sum_right[1].start()
    far_left[1].wait_recv()
    add_far(1, 1)
    sum_left[1].start()

    def total(m, p, lower):
        mine = acts[x, m, planes[p], pl.ds(half if lower else 0, half), 0:d].astype(F32)
        if lower:
            got = rs_dir[0, p, m].astype(F32) + rs_sum[1, p, m].astype(F32)
        else:
            got = rs_dir[1, p, m].astype(F32) + rs_sum[0, p, m].astype(F32)
        return (mine + got).astype(BF16)

    for c in (dir_right, dir_left, sum_right, sum_left):
        c[0].wait_recv()
    for m in range(3):
        acts[x, m, other, 0:half, 0:d] = total(m, 0, False)
        acts[x, m, other, half:fs, 0:d] = total(m, 0, True)
    swap_in = gcopy(12, acts.at[x, pl.ds(0, 2), other, full, pl.ds(0, d)], gin.at[h], to_partner)
    swap_out = gcopy(13, acts.at[x, 2, other, full, pl.ds(0, d)], gout.at[h], to_partner)
    swap_in.start()
    swap_out.start()

    for t in range(1, peers):
        u = target(t)
        dst = rows_buf.at[pl.ds(0, cap)]
        remote(dst, back.at[u], d_ssem.at[t], d_rsem.at[u], device(u)).wait_recv()
        remote(r_send.at[0], r_back.at[u], r_ssem.at[t], r_rsem.at[u], device(u)).wait_recv()
    for n in range(H):
        pc = place_col[n * toks : (n + 1) * toks, :]
        ids = lax.broadcasted_iota(jnp.int32, (toks, slots), 1)
        one = jnp.where((pc[:, 0:1] == ids) | (pc[:, 1:2] == ids), 1.0, 0.0).astype(BF16)
        gtok[:, n * d : (n + 1) * d] = dot_nn(one, back[...].reshape(slots, d)).astype(BF16)

    r_mine = r_back[:, 0, :]
    for k in range(2):
        pr = place_row[k : k + 1, :]
        expert = lax.shift_right_logical(pr, cap.bit_length() - 1)
        slot = lax.bitwise_and(pr, cap - 1)
        pick = jnp.where(lax.broadcasted_iota(jnp.int32, (peers, rows), 0) == expert, 1.0, 0.0)
        table = lax.dot_general(
            r_mine,
            pick,
            (((0,), (0,)), ((), ())),
            precision=lax.Precision.HIGHEST,
            preferred_element_type=F32,
        )
        lanes = lax.broadcasted_iota(jnp.int32, (128, rows), 0)
        value = jnp.sum(jnp.where(lanes == slot, table, 0.0), axis=0, keepdims=True)
        gprob[k : k + 1, :] = value / prob_row[k : k + 1, :]

    for c in (dir_right, dir_left, sum_right, sum_left):
        c[1].wait_recv()
    for m in range(2):
        gin[h, m, 0:half] = total(m, 1, False)
        gin[h, m, half:fs] = total(m, 1, True)
    gout[h, 0:half] = total(2, 1, False)
    gout[h, half:fs] = total(2, 1, True)

    for c in first + [f6, f7, f8, f9, f10, f11]:
        c.wait_send()
    for c in (far_right, far_left, dir_right, dir_left, sum_right, sum_left):
        c[0].wait_send()
        c[1].wait_send()
    for t in range(1, peers):
        xs_copy(t).wait_send()
        dst = rows_buf.at[pl.ds(0, cap)]
        remote(dst, back.at[0], d_ssem.at[t], d_rsem.at[0], device(source(t))).wait_send()
        remote(r_send.at[0], r_back.at[0], r_ssem.at[t], r_rsem.at[0], device(source(t))).wait_send()
    swap_in.wait()
    swap_out.wait()


def body(tokens, cotangent, expert_ids, slot_ids, route_probs, weights_in, weights_out):
    ng = lax.axis_size("expert")
    toks = tokens.shape[0]
    d = tokens.shape[1] // H
    fs = weights_in.shape[2]
    peers = NH * ng
    rows = toks * H
    cap = rows * 2 // peers
    slots = peers * cap
    half = fs // 2
    fc = NH * fs

    place = jnp.transpose(expert_ids * cap + slot_ids, (2, 1, 0)).reshape(2, rows)
    probs = jnp.transpose(route_probs, (2, 1, 0)).reshape(2, rows).astype(F32)
    place_col = jnp.transpose(place, (1, 0))

    vmem = pl.BlockSpec(memory_space=pltpu.VMEM)
    dma = pltpu.SemaphoreType.DMA
    gtok, gprob, gin, gout = pl.pallas_call(
        functools.partial(kernel, (ng, toks, d, fs, cap)),
        out_shape=(
            jax.ShapeDtypeStruct((toks, H * d), BF16),
            jax.ShapeDtypeStruct((2, rows), F32),
            jax.ShapeDtypeStruct((2, 2, fs, d), BF16),
            jax.ShapeDtypeStruct((2, fs, d), BF16),
        ),
        in_specs=[vmem] * 7,
        out_specs=(vmem,) * 4,
        scratch_shapes=[
            pltpu.VMEM((2 * rows, d), BF16),
            pltpu.VMEM((peers, 2, cap, d), BF16),
            pltpu.VMEM((peers, 2, cap, d), BF16),
            pltpu.VMEM((NX, 3, NH, fs, d), BF16),
            pltpu.VMEM((NX, 3, NH, fs, slots), BF16),
            pltpu.VMEM((slots, d), F32),
            pltpu.VMEM((8, slots), F32),
            pltpu.VMEM((2, 2, 3, half, d), BF16),
            pltpu.VMEM((2, 2, 3, half, d), BF16),
            pltpu.VMEM((2, 2, 3, half, d), BF16),
            pltpu.VMEM((peers, cap, d), BF16),
            pltpu.VMEM((peers, 8, 128), F32),
            pltpu.VMEM((peers, 8, 128), F32),
            dma((12,)),
            dma((12,)),
            dma((peers,)),
            dma((peers,)),
            dma((14,)),
            dma((14,)),
            dma((peers,)),
            dma((peers,)),
            dma((peers,)),
            dma((peers,)),
        ],
        compiler_params=pltpu.CompilerParams(
            collective_id=0, has_side_effects=True, vmem_limit_bytes=67_000_000
        ),
        name="moe_backward",
    )(tokens, cotangent, place, probs, place_col, weights_in, weights_out)
    grad_probs = jnp.transpose(gprob.reshape(2, H, toks), (2, 1, 0))
    return gtok, grad_probs, gin, gout


def solution(mesh):
    return jax.shard_map(
        body,
        mesh=mesh,
        in_specs=(
            P(("dp", "expert"), None),
            P(("dp", "expert"), None),
            P(("dp", "expert"), None, None),
            P(("dp", "expert"), None, None),
            P(("dp", "expert"), None, None),
            P("expert", None, "dp", None),
            P("expert", "dp", None),
        ),
        out_specs=(
            P(("dp", "expert"), None),
            P(("dp", "expert"), None, None),
            P("expert", None, "dp", None),
            P("expert", "dp", None),
        ),
        check_vma=False,
    )
```

```python
import functools

import jax
import jax.numpy as jnp
from jax import lax
from jax.experimental import pallas as pl
from jax.experimental.pallas import tpu as pltpu
from jax.sharding import PartitionSpec as P

H = 8
NX = 4
NH = 2
MESH = pl.DeviceIdType.MESH
F32 = jnp.float32
BF16 = jnp.bfloat16
BLOCKS = 4
FLIP = True
GRID = {16: (4, 2, 2), 2: (1, 1, 2)}


def dot_nn(a, b):
    return lax.dot_general(a, b, (((1,), (0,)), ((), ())), preferred_element_type=F32)


def dot_nt(a, b):
    return lax.dot_general(a, b, (((1,), (1,)), ((), ())), preferred_element_type=F32)


def dot_tn(a, b):
    return lax.dot_general(a, b, (((0,), (0,)), ((), ())), preferred_element_type=F32)


def send_order(nz, ny, nc):
    order = []
    for dc in range(nc):
        for s in range(nz):
            for dy in range(ny):
                order.append((dy, (3 * dy + s) % nz, dc))
    return order


def kernel(
    dims,
    tok,
    cot,
    ids_in,
    slots_in,
    probs_in,
    w_in,
    w_out,
    gtok,
    gprob,
    gin,
    gout,
    place_row,
    prob_row,
    gtok_buf,
    far_acc,
    rows_buf,
    xs_send,
    xs_all,
    wall,
    acts,
    dx,
    racc,
    rs_far,
    rs_sum,
    rs_dir,
    back,
    r_send,
    r_back,
    w_ssem,
    w_rsem,
    x_ssem,
    x_rsem,
    g_ssem,
    g_rsem,
    d_ssem,
    d_rsem,
    r_ssem,
    r_rsem,
    l_sem,
):
    ng, toks, d, fs, cap = dims
    nz, nyl, nc = GRID[ng]
    ny = NH * nyl
    peers = NH * ng
    rows = toks * H
    slots = peers * cap
    half = fs // 2
    fc = NH * fs
    jb = slots // BLOCKS
    per = peers // BLOCKS
    order = send_order(nz, ny, nc)

    dp = lax.axis_index("dp")
    g = lax.axis_index("expert")
    x = dp // NH
    h = dp % NH
    core = g % nc
    y = h * nyl + (g // nc) % nyl
    z = g // (nc * nyl)
    right = (x + 1) % NX
    left = (x + 3) % NX
    far = (x + 2) % NX
    other = 1 - h
    me = g * NH + h

    def place_of(ty, tz, tc):
        return ((tz * nyl + ty % nyl) * nc + tc) * NH + ty // nyl

    def target(t):
        dy, dz, dc = order[t]
        sign = 1 - 2 * core if FLIP else 1
        return place_of(
            (y + sign * dy + ny) % ny, (z + sign * dz + nz) % nz, (core + dc) % nc
        )

    def source(t):
        dy, dz, dc = order[t]
        tc = (core + dc) % nc
        sign = 1 - 2 * tc if FLIP else 1
        return place_of((y - sign * dy + ny) % ny, (z - sign * dz + nz) % nz, tc)

    def device(u):
        return (x * NH + u % NH, u // NH)

    def remote(src, dst, ssem, rsem, to):
        return pltpu.make_async_remote_copy(
            src_ref=src,
            dst_ref=dst,
            send_sem=ssem,
            recv_sem=rsem,
            device_id=to,
            device_id_type=MESH,
        )

    barrier = pltpu.get_barrier_semaphore()
    to_right = (right * NH + h, g)
    to_left = (left * NH + h, g)
    to_partner = (x * NH + other, g)
    for t in range(1, peers):
        pl.semaphore_signal(barrier, inc=1, device_id=device(target(t)), device_id_type=MESH)
    for to in (to_right, to_left):
        pl.semaphore_signal(barrier, inc=1, device_id=to, device_id_type=MESH)

    local = []
    for k, src in enumerate((tok, cot)):
        for n in range(H):
            dst = rows_buf.at[pl.ds((k * H + n) * toks, toks)]
            local.append((src.at[:, pl.ds(n * d, d)], dst))
    local.append((w_in.at[h], wall.at[x, pl.ds(0, 2), h]))
    local.append((w_out.at[h], wall.at[x, 2, h]))
    local = [pltpu.make_async_copy(a, b, l_sem.at[n]) for n, (a, b) in enumerate(local)]
    for c in local:
        c.start()
    place = ids_in[...] * cap + slots_in[...]
    probs = probs_in[...].astype(F32)
    for k in range(2):
        place_row[k : k + 1, :] = jnp.concatenate([place[n, k : k + 1] for n in range(H)], axis=1)
        prob_row[k : k + 1, :] = jnp.concatenate([probs[n, k : k + 1] for n in range(H)], axis=1)
    pl.semaphore_wait(barrier, peers + 1)

    def wcopy(k, src, dst, to):
        return remote(src, dst, w_ssem.at[k], w_rsem.at[k], to)

    first = [
        wcopy(0, w_in.at[other], wall.at[x, pl.ds(0, 2), h], to_partner),
        wcopy(1, w_out.at[other], wall.at[x, 2, h], to_partner),
        wcopy(2, w_in.at[h], wall.at[x, pl.ds(0, 2), h], to_right),
        wcopy(3, w_out.at[h], wall.at[x, 2, h], to_right),
        wcopy(4, w_in.at[h], wall.at[x, pl.ds(0, 2), h], to_left),
        wcopy(5, w_out.at[h], wall.at[x, 2, h], to_left),
    ]
    for c in first:
        c.start()

    for c in local:
        c.wait()

    pairs = nz * nyl
    width = min(2, pairs)
    span = NH * cap

    def xs_copy(t):
        u = target(t)
        return remote(xs_send.at[u], xs_all.at[t], x_ssem.at[t], x_rsem.at[t], device(u))

    for dc in range(nc):
        cc = (core + dc) % nc

        def dispatch(i, carry):
            row = lax.broadcasted_iota(jnp.int32, (width * span, rows), 0)
            ids = row + ((i * width * nc + cc) * span)
            if width == 2:
                ids = ids + jnp.where(row >= span, (nc - 1) * span, 0)
            hit0 = place_row[0:1, :] == ids
            hit1 = place_row[1:2, :] == ids
            one = jnp.where(hit0 | hit1, 1.0, 0.0).astype(BF16)
            wgt = jnp.where(hit0, prob_row[0:1, :], jnp.where(hit1, prob_row[1:2, :], 0.0))
            xr = dot_nn(one, rows_buf[0:rows, :]).astype(BF16)
            sr = dot_nn(wgt.astype(BF16), rows_buf[rows : 2 * rows, :]).astype(BF16)
            for j in range(width):
                e0 = ((i * width + j) * nc + cc) * NH
                for k in range(NH):
                    at = (j * NH + k) * cap
                    xs_send[e0 + k, 0] = xr[at : at + cap, :]
                    xs_send[e0 + k, 1] = sr[at : at + cap, :]
            return carry

        lax.fori_loop(0, pairs // width, dispatch, 0)
        for t in range(1, peers):
            if order[t][2] == dc:
                xs_copy(t).start()

    xs_all[0] = xs_send[me]
    racc[...] = jnp.zeros_like(racc)
    dx[...] = jnp.zeros_like(dx)

    def wforward(k, slot, part_rows, plane, to):
        ref = wall.at[slot, pl.ds(0, 3), plane, part_rows]
        return wcopy(k, ref, ref, to)

    top, bottom, full = pl.ds(0, half), pl.ds(half, half), pl.ds(0, fs)

    def xs_wait(i):
        for t in range(max(1, i * per), (i + 1) * per):
            xs_copy(t).wait_recv()

    def block(xc, i):
        at = pl.ds(pl.multiple_of(i * jb, jb), jb)
        some = pl.ds(i * per, per)
        xb = xs_all[some, 0].reshape(jb, d)
        sb = xs_all[some, 1].reshape(jb, d)
        wg = wall[xc, 0].reshape(fc, d)
        wu = wall[xc, 1].reshape(fc, d)
        wo = wall[xc, 2].reshape(fc, d)
        gate = dot_nt(wg, xb)
        up = dot_nt(wu, xb)
        dh = dot_nt(wo, sb)
        sg = 0.5 * jnp.tanh(0.5 * gate) + 0.5
        a = gate * sg
        du = dh * a
        dg = dh * up * (sg + a * (1.0 - sg))
        dgb = dg.astype(BF16)
        dub = du.astype(BF16)
        acts[xc, 0, :, :, at] = dgb.reshape(NH, fs, jb)
        acts[xc, 1, :, :, at] = dub.reshape(NH, fs, jb)
        acts[xc, 2, :, :, at] = (a * up).astype(BF16).reshape(NH, fs, jb)
        racc[:, at] += jnp.sum((du * up).reshape(fc // 8, 8, jb), axis=0)
        dx[at, :] += dot_tn(dgb, wg) + dot_tn(dub, wu)

    def sweep(count, xc_of, i_of):
        def step(n, carry):
            block(xc_of(n), i_of(n))
            return carry

        lax.fori_loop(0, count, step, 0)

    first[2].wait_recv()
    first[3].wait_recv()
    f6 = wforward(6, left, top, h, to_right)
    f6.start()
    first[4].wait_recv()
    first[5].wait_recv()
    f7 = wforward(7, right, bottom, h, to_left)
    f7.start()
    first[0].wait_recv()
    first[1].wait_recv()
    f8 = wforward(8, x, full, other, to_right)
    f8.start()
    f9 = wforward(9, x, full, other, to_left)
    f9.start()
    xs_wait(0)
    sweep(1, lambda n: x, lambda n: n * 0)
    f8.wait_recv()
    f10 = wforward(10, left, top, other, to_right)
    f10.start()
    f9.wait_recv()
    f11 = wforward(11, right, bottom, other, to_left)
    f11.start()
    sweep(2, lambda n: (x + 1 + 2 * n) % NX, lambda n: n * 0)
    xs_wait(1)
    sweep(3, lambda n: (x + jnp.where(n == 2, 3, n)) % NX, lambda n: n * 0 + 1)
    for c in (f6, f7, f10, f11):
        c.wait_recv()
    sweep(2, lambda n: far, lambda n: n)
    xs_wait(2)
    sweep(4, lambda n: (x + 2 + n) % NX, lambda n: n * 0 + 2)

    before = slots - jb
    for m in range(3):
        far_acc[m] = dot_nn(
            acts[far, m, :, :, 0:before].reshape(fc, before),
            xs_all[0 : peers - per, m // 2].reshape(before, d),
        )
    xs_wait(3)

    def give(i):
        for k in range(per):
            t = i * per + k
            dst = rows_buf.at[pl.ds(t * cap, cap)]
            if t:
                u = source(t)
                remote(dst, back.at[me], d_ssem.at[t], d_rsem.at[me], device(u)).start()
                remote(r_send.at[t], r_back.at[me], r_ssem.at[t], r_rsem.at[me], device(u)).start()
            else:
                back[me] = rows_buf[0:cap, :]
                r_back[me] = r_send[0]

    def finish(i):
        rows_buf[i * jb : (i + 1) * jb, :] = dx[i * jb : (i + 1) * jb, :].astype(BF16)
        r_row = jnp.sum(racc[:, i * jb : (i + 1) * jb], axis=0, keepdims=True)
        for k in range(per):
            v = r_row[:, k * cap : (k + 1) * cap]
            r_send[i * per + k] = jnp.broadcast_to(jnp.concatenate([v, v], axis=1), (8, 128))

    planes = (other, h)

    def gcopy(k, src, dst, to):
        return remote(src, dst, g_ssem.at[k], g_rsem.at[k], to)

    def piece(xc, part_rows, plane):
        return acts.at[xc, pl.ds(0, 3), plane, part_rows, pl.ds(0, d)]

    far_right = [gcopy(p, piece(far, top, planes[p]), rs_far.at[0, p], to_right) for p in (0, 1)]
    far_left = [
        gcopy(2 + p, piece(far, bottom, planes[p]), rs_far.at[1, p], to_left) for p in (0, 1)
    ]
    dir_right = [
        gcopy(4 + p, piece(right, bottom, planes[p]), rs_dir.at[0, p], to_right) for p in (0, 1)
    ]
    dir_left = [
        gcopy(6 + p, piece(left, top, planes[p]), rs_dir.at[1, p], to_left) for p in (0, 1)
    ]
    sum_right = [
        gcopy(8 + p, piece(right, top, planes[p]), rs_sum.at[0, p], to_right) for p in (0, 1)
    ]
    sum_left = [
        gcopy(10 + p, piece(left, bottom, planes[p]), rs_sum.at[1, p], to_left) for p in (0, 1)
    ]

    def weight_grads(xc):
        xa = xs_all[:, 0].reshape(slots, d)
        sa = xs_all[:, 1].reshape(slots, d)
        for m, against in ((0, xa), (1, xa), (2, sa)):
            grad = dot_nn(acts[xc, m].reshape(fc, slots), against)
            acts[xc, m, :, :, 0:d] = grad.astype(BF16).reshape(NH, fs, d)

    def add_far(side, p):
        xc, part_rows = (right, top) if side == 0 else (left, bottom)
        for m in range(3):
            mine = acts[xc, m, planes[p], part_rows, 0:d].astype(F32)
            acts[xc, m, planes[p], part_rows, 0:d] = (
                rs_far[side, p, m].astype(F32) + mine
            ).astype(BF16)

    block(far, BLOCKS - 1)
    for m in range(3):
        grad = far_acc[m] + dot_nn(
            acts[far, m, :, :, before:slots].reshape(fc, jb),
            xs_all[peers - per : peers, m // 2].reshape(jb, d),
        )
        acts[far, m, :, :, 0:d] = grad.astype(BF16).reshape(NH, fs, d)
    for p in (0, 1):
        far_right[p].start()
        far_left[p].start()
    for i in range(BLOCKS - 1):
        finish(i)
        give(i)

    def last(n, carry):
        xc = (x + jnp.where(n == 0, 1, jnp.where(n == 1, 3, 0))) % NX
        block(xc, BLOCKS - 1)

        @pl.when(n == 2)
        def _():
            finish(BLOCKS - 1)
            give(BLOCKS - 1)

        weight_grads(xc)

        @pl.when(n == 0)
        def _():
            dir_right[0].start()

        @pl.when(n == 1)
        def _():
            dir_left[0].start()
            far_right[0].wait_recv()
            add_far(0, 0)
            sum_right[0].start()
            dir_right[1].start()
            far_left[0].wait_recv()
            add_far(1, 0)
            sum_left[0].start()
            dir_left[1].start()

        return carry

    lax.fori_loop(0, NX - 1, last, 0)
    far_right[1].wait_recv()
    add_far(0, 1)
    sum_right[1].start()
    far_left[1].wait_recv()
    add_far(1, 1)
    sum_left[1].start()

    def total(m, p, lower):
        mine = acts[x, m, planes[p], pl.ds(half if lower else 0, half), 0:d].astype(F32)
        if lower:
            got = rs_dir[0, p, m].astype(F32) + rs_sum[1, p, m].astype(F32)
        else:
            got = rs_dir[1, p, m].astype(F32) + rs_sum[0, p, m].astype(F32)
        return (mine + got).astype(BF16)

    for c in (dir_right, dir_left, sum_right, sum_left):
        c[0].wait_recv()
    for m in range(3):
        acts[x, m, other, 0:half, 0:d] = total(m, 0, False)
        acts[x, m, other, half:fs, 0:d] = total(m, 0, True)
    swap_in = gcopy(12, acts.at[x, pl.ds(0, 2), other, full, pl.ds(0, d)], gin.at[h], to_partner)
    swap_out = gcopy(13, acts.at[x, 2, other, full, pl.ds(0, d)], gout.at[h], to_partner)
    swap_in.start()
    swap_out.start()

    for t in range(1, peers):
        u = target(t)
        dst = rows_buf.at[pl.ds(0, cap)]
        remote(dst, back.at[u], d_ssem.at[t], d_rsem.at[u], device(u)).wait_recv()
        remote(r_send.at[0], r_back.at[u], r_ssem.at[t], r_rsem.at[u], device(u)).wait_recv()
    flat = jnp.concatenate(
        [place_row[k : k + 1, n * toks : (n + 1) * toks] for n in range(H) for k in range(2)],
        axis=0,
    )
    cols = jnp.transpose(flat.astype(F32), (1, 0)).astype(jnp.int32)
    ids = lax.broadcasted_iota(jnp.int32, (toks, slots), 1)
    for n in range(H):
        hit = (cols[:, 2 * n : 2 * n + 1] == ids) | (cols[:, 2 * n + 1 : 2 * n + 2] == ids)
        one = jnp.where(hit, 1.0, 0.0).astype(BF16)
        grad = dot_nn(one, back[...].reshape(slots, d))
        gtok_buf[:, n * d : (n + 1) * d] = grad.astype(BF16)
    tok_out = pltpu.make_async_copy(gtok_buf, gtok, l_sem.at[2 * H + 2])
    tok_out.start()

    r_mine = r_back[:, 0, :]
    for k in range(2):
        pr = place_row[k : k + 1, :]
        expert = lax.shift_right_logical(pr, cap.bit_length() - 1)
        slot = lax.bitwise_and(pr, cap - 1)
        pick = jnp.where(lax.broadcasted_iota(jnp.int32, (peers, rows), 0) == expert, 1.0, 0.0)
        table = lax.dot_general(
            r_mine,
            pick,
            (((0,), (0,)), ((), ())),
            precision=lax.Precision.HIGHEST,
            preferred_element_type=F32,
        )
        lanes = lax.broadcasted_iota(jnp.int32, (128, rows), 0)
        value = jnp.sum(jnp.where(lanes == slot, table, 0.0), axis=0, keepdims=True)
        ratio = value / prob_row[k : k + 1, :]
        for n in range(H):
            gprob[n, k : k + 1, :] = ratio[:, n * toks : (n + 1) * toks]

    for c in (dir_right, dir_left, sum_right, sum_left):
        c[1].wait_recv()
    for m in range(2):
        gin[h, m, 0:half] = total(m, 1, False)
        gin[h, m, half:fs] = total(m, 1, True)
    gout[h, 0:half] = total(2, 1, False)
    gout[h, half:fs] = total(2, 1, True)

    tok_out.wait()
    for c in first + [f6, f7, f8, f9, f10, f11]:
        c.wait_send()
    for c in (far_right, far_left, dir_right, dir_left, sum_right, sum_left):
        c[0].wait_send()
        c[1].wait_send()
    for t in range(1, peers):
        xs_copy(t).wait_send()
        dst = rows_buf.at[pl.ds(0, cap)]
        remote(dst, back.at[0], d_ssem.at[t], d_rsem.at[0], device(source(t))).wait_send()
        remote(r_send.at[0], r_back.at[0], r_ssem.at[t], r_rsem.at[0], device(source(t))).wait_send()
    swap_in.wait()
    swap_out.wait()


def copy_kernel(*refs):
    ins, outs, bufs, (in_sem, out_sem) = refs[0:4], refs[4:8], refs[8:12], refs[12:14]
    count = ins[0].shape[0] // 4
    parts = [(0, pl.ds(k * count, count)) for k in range(4)]
    parts += [(2, pl.ds(0, 1)), (2, pl.ds(1, 1)), (3, pl.ds(0, 1)), (3, pl.ds(1, 1))]
    parts += [(1, pl.ds(0, ins[1].shape[0]))]
    moves = []
    for n, (a, at) in enumerate(parts):
        moves.append(
            (
                pltpu.make_async_copy(ins[a].at[at], bufs[a].at[at], in_sem.at[n]),
                pltpu.make_async_copy(bufs[a].at[at], outs[a].at[at], out_sem.at[n]),
            )
        )
    for into, _ in moves:
        into.start()
    for into, out in moves:
        into.wait()
        out.start()
    for _, out in moves:
        out.wait()


def body(tokens, cotangent, expert_ids, slot_ids, route_probs, weights_in, weights_out):
    ng = lax.axis_size("expert")
    toks = tokens.shape[0]
    d = tokens.shape[1] // H
    fs = weights_in.shape[2]
    peers = NH * ng
    rows = toks * H
    cap = rows * 2 // peers
    slots = peers * cap
    half = fs // 2
    fc = NH * fs

    vmem = pl.BlockSpec(memory_space=pltpu.VMEM)
    anywhere = pl.BlockSpec(memory_space=pl.ANY)
    dma = pltpu.SemaphoreType.DMA
    gtok, gprob, gin, gout = pl.pallas_call(
        functools.partial(kernel, (ng, toks, d, fs, cap)),
        out_shape=(
            jax.ShapeDtypeStruct((toks, H * d), BF16),
            jax.ShapeDtypeStruct((H, 2, toks), F32),
            jax.ShapeDtypeStruct((2, 2, fs, d), BF16),
            jax.ShapeDtypeStruct((2, fs, d), BF16),
        ),
        in_specs=[anywhere] * 2 + [vmem] * 3 + [anywhere] * 2,
        out_specs=(anywhere, vmem, vmem, vmem),
        scratch_shapes=[
            pltpu.VMEM((2, rows), jnp.int32),
            pltpu.VMEM((2, rows), F32),
            pltpu.VMEM((toks, H * d), BF16),
            pltpu.VMEM((3, fc, d), F32),
            pltpu.VMEM((2 * rows, d), BF16),
            pltpu.VMEM((peers, 2, cap, d), BF16),
            pltpu.VMEM((peers, 2, cap, d), BF16),
            pltpu.VMEM((NX, 3, NH, fs, d), BF16),
            pltpu.VMEM((NX, 3, NH, fs, slots), BF16),
            pltpu.VMEM((slots, d), F32),
            pltpu.VMEM((8, slots), F32),
            pltpu.VMEM((2, 2, 3, half, d), BF16),
            pltpu.VMEM((2, 2, 3, half, d), BF16),
            pltpu.VMEM((2, 2, 3, half, d), BF16),
            pltpu.VMEM((peers, cap, d), BF16),
            pltpu.VMEM((peers, 8, 128), F32),
            pltpu.VMEM((peers, 8, 128), F32),
            dma((12,)),
            dma((12,)),
            dma((peers,)),
            dma((peers,)),
            dma((14,)),
            dma((14,)),
            dma((peers,)),
            dma((peers,)),
            dma((peers,)),
            dma((peers,)),
            dma((2 * H + 3,)),
        ],
        compiler_params=pltpu.CompilerParams(
            collective_id=0, has_side_effects=True, vmem_limit_bytes=67_000_000
        ),
        name="moe_backward",
    )(
        tokens,
        cotangent,
        jnp.transpose(expert_ids, (1, 2, 0)),
        jnp.transpose(slot_ids, (1, 2, 0)),
        jnp.transpose(route_probs, (1, 2, 0)),
        weights_in,
        weights_out,
    )
    gtok, gprob, gin, gout = pl.pallas_call(
        copy_kernel,
        out_shape=tuple(jax.ShapeDtypeStruct(a.shape, a.dtype) for a in (gtok, gprob, gin, gout)),
        in_specs=[anywhere] * 4,
        out_specs=(anywhere,) * 4,
        scratch_shapes=[pltpu.VMEM(a.shape, a.dtype) for a in (gtok, gprob, gin, gout)]
        + [dma((10,)), dma((10,))],
        name="results",
    )(gtok, gprob, gin, gout)
    return gtok, jnp.transpose(gprob, (2, 0, 1)), gin, gout


def solution(mesh):
    return jax.shard_map(
        body,
        mesh=mesh,
        in_specs=(
            P(("dp", "expert"), None),
            P(("dp", "expert"), None),
            P(("dp", "expert"), None, None),
            P(("dp", "expert"), None, None),
            P(("dp", "expert"), None, None),
            P("expert", None, "dp", None),
            P("expert", "dp", None),
        ),
        out_specs=(
            P(("dp", "expert"), None),
            P(("dp", "expert"), None, None),
            P("expert", None, "dp", None),
            P("expert", "dp", None),
        ),
        check_vma=False,
    )
```

```python
import functools

import jax
import jax.numpy as jnp
from jax import lax
from jax.experimental import pallas as pl
from jax.experimental.pallas import tpu as pltpu
from jax.sharding import PartitionSpec as P

H = 8
NX = 4
NH = 2
MESH = pl.DeviceIdType.MESH
F32 = jnp.float32
BF16 = jnp.bfloat16
BLOCKS = 4
FLIP = True
GRID = {16: (4, 2, 2), 2: (1, 1, 2)}


def dot_nn(a, b):
    return lax.dot_general(a, b, (((1,), (0,)), ((), ())), preferred_element_type=F32)


def dot_nt(a, b):
    return lax.dot_general(a, b, (((1,), (1,)), ((), ())), preferred_element_type=F32)


def dot_tn(a, b):
    return lax.dot_general(a, b, (((0,), (0,)), ((), ())), preferred_element_type=F32)


def send_order(nz, ny, nc):
    order = []
    for dc in range(nc):
        for s in range(nz):
            for dy in range(ny):
                order.append((dy, (3 * dy + s) % nz, dc))
    return order


def kernel(
    dims,
    tok,
    cot,
    ids_in,
    slots_in,
    probs_in,
    w_in,
    w_out,
    gtok,
    gprob,
    gin,
    gout,
    place_row,
    prob_row,
    far_acc,
    rows_buf,
    xs_send,
    xs_all,
    wall,
    acts,
    dx,
    racc,
    rs_far,
    rs_sum,
    rs_dir,
    back,
    r_send,
    r_back,
    w_ssem,
    w_rsem,
    x_ssem,
    x_rsem,
    g_ssem,
    g_rsem,
    d_ssem,
    d_rsem,
    r_ssem,
    r_rsem,
    l_sem,
):
    ng, toks, d, fs, cap = dims
    nz, nyl, nc = GRID[ng]
    ny = NH * nyl
    peers = NH * ng
    rows = toks * H
    slots = peers * cap
    half = fs // 2
    fc = NH * fs
    jb = slots // BLOCKS
    per = peers // BLOCKS
    order = send_order(nz, ny, nc)

    dp = lax.axis_index("dp")
    g = lax.axis_index("expert")
    x = dp // NH
    h = dp % NH
    core = g % nc
    y = h * nyl + (g // nc) % nyl
    z = g // (nc * nyl)
    right = (x + 1) % NX
    left = (x + 3) % NX
    far = (x + 2) % NX
    other = 1 - h
    me = g * NH + h

    def place_of(ty, tz, tc):
        return ((tz * nyl + ty % nyl) * nc + tc) * NH + ty // nyl

    def target(t):
        dy, dz, dc = order[t]
        sign = 1 - 2 * core if FLIP else 1
        return place_of(
            (y + sign * dy + ny) % ny, (z + sign * dz + nz) % nz, (core + dc) % nc
        )

    def source(t):
        dy, dz, dc = order[t]
        tc = (core + dc) % nc
        sign = 1 - 2 * tc if FLIP else 1
        return place_of((y - sign * dy + ny) % ny, (z - sign * dz + nz) % nz, tc)

    def device(u):
        return (x * NH + u % NH, u // NH)

    def remote(src, dst, ssem, rsem, to):
        return pltpu.make_async_remote_copy(
            src_ref=src,
            dst_ref=dst,
            send_sem=ssem,
            recv_sem=rsem,
            device_id=to,
            device_id_type=MESH,
        )

    barrier = pltpu.get_barrier_semaphore()
    to_right = (right * NH + h, g)
    to_left = (left * NH + h, g)
    to_partner = (x * NH + other, g)
    for t in range(1, peers):
        pl.semaphore_signal(barrier, inc=1, device_id=device(target(t)), device_id_type=MESH)
    for to in (to_right, to_left):
        pl.semaphore_signal(barrier, inc=1, device_id=to, device_id_type=MESH)

    local = []
    for k, src in enumerate((tok, cot)):
        for n in range(H):
            dst = rows_buf.at[pl.ds((k * H + n) * toks, toks)]
            local.append((src.at[:, pl.ds(n * d, d)], dst))
    local.append((w_in.at[h], wall.at[x, pl.ds(0, 2), h]))
    local.append((w_out.at[h], wall.at[x, 2, h]))
    local = [pltpu.make_async_copy(a, b, l_sem.at[n]) for n, (a, b) in enumerate(local)]
    for c in local:
        c.start()
    place = ids_in[...] * cap + slots_in[...]
    probs = probs_in[...].astype(F32)
    for k in range(2):
        place_row[k : k + 1, :] = jnp.concatenate([place[n, k : k + 1] for n in range(H)], axis=1)
        prob_row[k : k + 1, :] = jnp.concatenate([probs[n, k : k + 1] for n in range(H)], axis=1)
    pl.semaphore_wait(barrier, peers + 1)

    def wcopy(k, src, dst, to):
        return remote(src, dst, w_ssem.at[k], w_rsem.at[k], to)

    first = [
        wcopy(0, w_in.at[other], wall.at[x, pl.ds(0, 2), h], to_partner),
        wcopy(1, w_out.at[other], wall.at[x, 2, h], to_partner),
        wcopy(2, w_in.at[h], wall.at[x, pl.ds(0, 2), h], to_right),
        wcopy(3, w_out.at[h], wall.at[x, 2, h], to_right),
        wcopy(4, w_in.at[h], wall.at[x, pl.ds(0, 2), h], to_left),
        wcopy(5, w_out.at[h], wall.at[x, 2, h], to_left),
    ]
    for c in first:
        c.start()

    for c in local:
        c.wait()

    pairs = nz * nyl
    width = min(2, pairs)
    span = NH * cap

    def xs_copy(t):
        u = target(t)
        return remote(xs_send.at[u], xs_all.at[t], x_ssem.at[t], x_rsem.at[t], device(u))

    for dc in range(nc):
        cc = (core + dc) % nc

        def dispatch(i, carry):
            row = lax.broadcasted_iota(jnp.int32, (width * span, rows), 0)
            ids = row + ((i * width * nc + cc) * span)
            if width == 2:
                ids = ids + jnp.where(row >= span, (nc - 1) * span, 0)
            hit0 = place_row[0:1, :] == ids
            hit1 = place_row[1:2, :] == ids
            one = jnp.where(hit0 | hit1, 1.0, 0.0).astype(BF16)
            wgt = jnp.where(hit0, prob_row[0:1, :], jnp.where(hit1, prob_row[1:2, :], 0.0))
            xr = dot_nn(one, rows_buf[0:rows, :]).astype(BF16)
            sr = dot_nn(wgt.astype(BF16), rows_buf[rows : 2 * rows, :]).astype(BF16)
            for j in range(width):
                e0 = ((i * width + j) * nc + cc) * NH
                for k in range(NH):
                    at = (j * NH + k) * cap
                    xs_send[e0 + k, 0] = xr[at : at + cap, :]
                    xs_send[e0 + k, 1] = sr[at : at + cap, :]
            return carry

        lax.fori_loop(0, pairs // width, dispatch, 0)
        for t in range(1, peers):
            if order[t][2] == dc:
                xs_copy(t).start()

    xs_all[0] = xs_send[me]
    racc[...] = jnp.zeros_like(racc)
    dx[...] = jnp.zeros_like(dx)

    def wforward(k, slot, part_rows, plane, to):
        ref = wall.at[slot, pl.ds(0, 3), plane, part_rows]
        return wcopy(k, ref, ref, to)

    top, bottom, full = pl.ds(0, half), pl.ds(half, half), pl.ds(0, fs)

    def xs_wait(i, share=1):
        count = per // share
        for t in range(max(1, i * count), (i + 1) * count):
            xs_copy(t).wait_recv()

    def block(xc, i, share=1):
        per, jb = peers // BLOCKS // share, slots // BLOCKS // share
        at = pl.ds(pl.multiple_of(i * jb, jb), jb)
        some = pl.ds(i * per, per)
        xb = xs_all[some, 0].reshape(jb, d)
        sb = xs_all[some, 1].reshape(jb, d)
        wg = wall[xc, 0].reshape(fc, d)
        wu = wall[xc, 1].reshape(fc, d)
        wo = wall[xc, 2].reshape(fc, d)
        gate = dot_nt(wg, xb)
        up = dot_nt(wu, xb)
        dh = dot_nt(wo, sb)
        sg = 0.5 * jnp.tanh(0.5 * gate) + 0.5
        a = gate * sg
        du = dh * a
        dg = dh * up * (sg + a * (1.0 - sg))
        dgb = dg.astype(BF16)
        dub = du.astype(BF16)
        acts[xc, 0, :, :, at] = dgb.reshape(NH, fs, jb)
        acts[xc, 1, :, :, at] = dub.reshape(NH, fs, jb)
        acts[xc, 2, :, :, at] = (a * up).astype(BF16).reshape(NH, fs, jb)
        racc[:, at] += jnp.sum((du * up).reshape(fc // 8, 8, jb), axis=0)
        dx[at, :] += dot_tn(dgb, wg) + dot_tn(dub, wu)

    def sweep(count, xc_of, i_of):
        def step(n, carry):
            block(xc_of(n), i_of(n))
            return carry

        lax.fori_loop(0, count, step, 0)

    first[2].wait_recv()
    first[3].wait_recv()
    f6 = wforward(6, left, top, h, to_right)
    f6.start()
    first[4].wait_recv()
    first[5].wait_recv()
    f7 = wforward(7, right, bottom, h, to_left)
    f7.start()
    first[0].wait_recv()
    first[1].wait_recv()
    f8 = wforward(8, x, full, other, to_right)
    f8.start()
    f9 = wforward(9, x, full, other, to_left)
    f9.start()
    xs_wait(0)
    sweep(1, lambda n: x, lambda n: n * 0)
    f8.wait_recv()
    f10 = wforward(10, left, top, other, to_right)
    f10.start()
    f9.wait_recv()
    f11 = wforward(11, right, bottom, other, to_left)
    f11.start()
    sweep(2, lambda n: (x + 1 + 2 * n) % NX, lambda n: n * 0)
    xs_wait(1)
    sweep(3, lambda n: (x + jnp.where(n == 2, 3, n)) % NX, lambda n: n * 0 + 1)
    for c in (f6, f7, f10, f11):
        c.wait_recv()
    sweep(2, lambda n: far, lambda n: n)
    xs_wait(2)
    sweep(4, lambda n: (x + 2 + n) % NX, lambda n: n * 0 + 2)

    before = slots - jb
    for m in range(3):
        far_acc[m] = dot_nn(
            acts[far, m, :, :, 0:before].reshape(fc, before),
            xs_all[0 : peers - per, m // 2].reshape(before, d),
        )
    def give(i):
        for k in range(per):
            t = i * per + k
            dst = rows_buf.at[pl.ds(t * cap, cap)]
            if t:
                u = source(t)
                remote(dst, back.at[me], d_ssem.at[t], d_rsem.at[me], device(u)).start()
                remote(r_send.at[t], r_back.at[me], r_ssem.at[t], r_rsem.at[me], device(u)).start()
            else:
                back[me] = rows_buf[0:cap, :]
                r_back[me] = r_send[0]

    def finish(i):
        rows_buf[i * jb : (i + 1) * jb, :] = dx[i * jb : (i + 1) * jb, :].astype(BF16)
        r_row = jnp.sum(racc[:, i * jb : (i + 1) * jb], axis=0, keepdims=True)
        for k in range(per):
            v = r_row[:, k * cap : (k + 1) * cap]
            r_send[i * per + k] = jnp.broadcast_to(jnp.concatenate([v, v], axis=1), (8, 128))

    planes = (other, h)

    def gcopy(k, src, dst, to):
        return remote(src, dst, g_ssem.at[k], g_rsem.at[k], to)

    def piece(xc, part_rows, plane):
        return acts.at[xc, pl.ds(0, 3), plane, part_rows, pl.ds(0, d)]

    far_right = [gcopy(p, piece(far, top, planes[p]), rs_far.at[0, p], to_right) for p in (0, 1)]
    far_left = [
        gcopy(2 + p, piece(far, bottom, planes[p]), rs_far.at[1, p], to_left) for p in (0, 1)
    ]
    dir_right = [
        gcopy(4 + p, piece(right, bottom, planes[p]), rs_dir.at[0, p], to_right) for p in (0, 1)
    ]
    dir_left = [
        gcopy(6 + p, piece(left, top, planes[p]), rs_dir.at[1, p], to_left) for p in (0, 1)
    ]
    sum_right = [
        gcopy(8 + p, piece(right, top, planes[p]), rs_sum.at[0, p], to_right) for p in (0, 1)
    ]
    sum_left = [
        gcopy(10 + p, piece(left, bottom, planes[p]), rs_sum.at[1, p], to_left) for p in (0, 1)
    ]

    def weight_grads(xc):
        xa = xs_all[:, 0].reshape(slots, d)
        sa = xs_all[:, 1].reshape(slots, d)
        for m, against in ((0, xa), (1, xa), (2, sa)):
            grad = dot_nn(acts[xc, m].reshape(fc, slots), against)
            acts[xc, m, :, :, 0:d] = grad.astype(BF16).reshape(NH, fs, d)

    def add_far(side, p):
        xc, part_rows = (right, top) if side == 0 else (left, bottom)
        for m in range(3):
            mine = acts[xc, m, planes[p], part_rows, 0:d].astype(F32)
            acts[xc, m, planes[p], part_rows, 0:d] = (
                rs_far[side, p, m].astype(F32) + mine
            ).astype(BF16)

    share = min(2, per)
    for i in range((BLOCKS - 1) * share, BLOCKS * share):
        xs_wait(i, share)
        block(far, i, share)
    for m in range(3):
        grad = far_acc[m] + dot_nn(
            acts[far, m, :, :, before:slots].reshape(fc, jb),
            xs_all[peers - per : peers, m // 2].reshape(jb, d),
        )
        acts[far, m, :, :, 0:d] = grad.astype(BF16).reshape(NH, fs, d)
    for p in (0, 1):
        far_right[p].start()
        far_left[p].start()
    for i in range(BLOCKS - 1):
        finish(i)
        give(i)

    def last(n, carry):
        xc = (x + jnp.where(n == 0, 1, jnp.where(n == 1, 3, 0))) % NX
        block(xc, BLOCKS - 1)

        @pl.when(n == 2)
        def _():
            finish(BLOCKS - 1)
            give(BLOCKS - 1)

        weight_grads(xc)

        @pl.when(n == 0)
        def _():
            dir_right[0].start()

        @pl.when(n == 1)
        def _():
            dir_left[0].start()
            far_right[0].wait_recv()
            add_far(0, 0)
            sum_right[0].start()
            dir_right[1].start()
            far_left[0].wait_recv()
            add_far(1, 0)
            sum_left[0].start()
            dir_left[1].start()

        return carry

    lax.fori_loop(0, NX - 1, last, 0)
    far_right[1].wait_recv()
    add_far(0, 1)
    sum_right[1].start()
    far_left[1].wait_recv()
    add_far(1, 1)
    sum_left[1].start()

    def total(m, p, lower):
        mine = acts[x, m, planes[p], pl.ds(half if lower else 0, half), 0:d].astype(F32)
        if lower:
            got = rs_dir[0, p, m].astype(F32) + rs_sum[1, p, m].astype(F32)
        else:
            got = rs_dir[1, p, m].astype(F32) + rs_sum[0, p, m].astype(F32)
        return (mine + got).astype(BF16)

    for c in (dir_right, dir_left, sum_right, sum_left):
        c[0].wait_recv()
    for m in range(3):
        acts[x, m, other, 0:half, 0:d] = total(m, 0, False)
        acts[x, m, other, half:fs, 0:d] = total(m, 0, True)
    swap_in = gcopy(12, acts.at[x, pl.ds(0, 2), other, full, pl.ds(0, d)], gin.at[h], to_partner)
    swap_out = gcopy(13, acts.at[x, 2, other, full, pl.ds(0, d)], gout.at[h], to_partner)
    swap_in.start()
    swap_out.start()

    for t in range(1, peers):
        u = target(t)
        dst = rows_buf.at[pl.ds(0, cap)]
        remote(dst, back.at[u], d_ssem.at[t], d_rsem.at[u], device(u)).wait_recv()
        remote(r_send.at[0], r_back.at[u], r_ssem.at[t], r_rsem.at[u], device(u)).wait_recv()
    flat = jnp.concatenate(
        [place_row[k : k + 1, n * toks : (n + 1) * toks] for n in range(H) for k in range(2)],
        axis=0,
    )
    cols = jnp.transpose(flat.astype(F32), (1, 0)).astype(jnp.int32)
    ids = lax.broadcasted_iota(jnp.int32, (toks, slots), 1)
    for n in range(H):
        hit = (cols[:, 2 * n : 2 * n + 1] == ids) | (cols[:, 2 * n + 1 : 2 * n + 2] == ids)
        one = jnp.where(hit, 1.0, 0.0).astype(BF16)
        grad = dot_nn(one, back[...].reshape(slots, d))
        gtok[:, n * d : (n + 1) * d] = grad.astype(BF16)

    r_mine = r_back[:, 0, :]
    for k in range(2):
        pr = place_row[k : k + 1, :]
        expert = lax.shift_right_logical(pr, cap.bit_length() - 1)
        slot = lax.bitwise_and(pr, cap - 1)
        pick = jnp.where(lax.broadcasted_iota(jnp.int32, (peers, rows), 0) == expert, 1.0, 0.0)
        table = lax.dot_general(
            r_mine,
            pick,
            (((0,), (0,)), ((), ())),
            precision=lax.Precision.HIGHEST,
            preferred_element_type=F32,
        )
        lanes = lax.broadcasted_iota(jnp.int32, (128, rows), 0)
        value = jnp.sum(jnp.where(lanes == slot, table, 0.0), axis=0, keepdims=True)
        ratio = value / prob_row[k : k + 1, :]
        for n in range(H):
            gprob[n, k : k + 1, :] = ratio[:, n * toks : (n + 1) * toks]


    for c in (dir_right, dir_left, sum_right, sum_left):
        c[1].wait_recv()
    for m in range(2):
        gin[h, m, 0:half] = total(m, 1, False)
        gin[h, m, half:fs] = total(m, 1, True)
    gout[h, 0:half] = total(2, 1, False)
    gout[h, half:fs] = total(2, 1, True)

    for c in first + [f6, f7, f8, f9, f10, f11]:
        c.wait_send()
    for c in (far_right, far_left, dir_right, dir_left, sum_right, sum_left):
        c[0].wait_send()
        c[1].wait_send()
    for t in range(1, peers):
        xs_copy(t).wait_send()
        dst = rows_buf.at[pl.ds(0, cap)]
        remote(dst, back.at[0], d_ssem.at[t], d_rsem.at[0], device(source(t))).wait_send()
        remote(r_send.at[0], r_back.at[0], r_ssem.at[t], r_rsem.at[0], device(source(t))).wait_send()
    swap_in.wait()
    swap_out.wait()


def copy_kernel(*refs):
    ins, outs, sem = refs[0:4], refs[4:8], refs[8]
    moves = [pltpu.make_async_copy(ins[n], outs[n], sem.at[n]) for n in range(4)]
    for c in moves:
        c.start()
    for c in moves:
        c.wait()


def body(tokens, cotangent, expert_ids, slot_ids, route_probs, weights_in, weights_out):
    ng = lax.axis_size("expert")
    toks = tokens.shape[0]
    d = tokens.shape[1] // H
    fs = weights_in.shape[2]
    peers = NH * ng
    rows = toks * H
    cap = rows * 2 // peers
    slots = peers * cap
    half = fs // 2
    fc = NH * fs

    vmem = pl.BlockSpec(memory_space=pltpu.VMEM)
    anywhere = pl.BlockSpec(memory_space=pl.ANY)
    dma = pltpu.SemaphoreType.DMA
    gtok, gprob, gin, gout = pl.pallas_call(
        functools.partial(kernel, (ng, toks, d, fs, cap)),
        out_shape=(
            pltpu.VMEM((toks, H * d), BF16),
            pltpu.VMEM((H, 2, toks), F32),
            pltpu.VMEM((2, 2, fs, d), BF16),
            pltpu.VMEM((2, fs, d), BF16),
        ),
        in_specs=[anywhere] * 2 + [vmem] * 3 + [anywhere] * 2,
        out_specs=(vmem,) * 4,
        scratch_shapes=[
            pltpu.VMEM((2, rows), jnp.int32),
            pltpu.VMEM((2, rows), F32),
            pltpu.VMEM((3, fc, d), F32),
            pltpu.VMEM((2 * rows, d), BF16),
            pltpu.VMEM((peers, 2, cap, d), BF16),
            pltpu.VMEM((peers, 2, cap, d), BF16),
            pltpu.VMEM((NX, 3, NH, fs, d), BF16),
            pltpu.VMEM((NX, 3, NH, fs, slots), BF16),
            pltpu.VMEM((slots, d), F32),
            pltpu.VMEM((8, slots), F32),
            pltpu.VMEM((2, 2, 3, half, d), BF16),
            pltpu.VMEM((2, 2, 3, half, d), BF16),
            pltpu.VMEM((2, 2, 3, half, d), BF16),
            pltpu.VMEM((peers, cap, d), BF16),
            pltpu.VMEM((peers, 8, 128), F32),
            pltpu.VMEM((peers, 8, 128), F32),
            dma((12,)),
            dma((12,)),
            dma((peers,)),
            dma((peers,)),
            dma((14,)),
            dma((14,)),
            dma((peers,)),
            dma((peers,)),
            dma((peers,)),
            dma((peers,)),
            dma((2 * H + 2,)),
        ],
        compiler_params=pltpu.CompilerParams(
            collective_id=0, has_side_effects=True, vmem_limit_bytes=60_000_000
        ),
        name="moe_backward",
    )(
        tokens,
        cotangent,
        jnp.transpose(expert_ids, (1, 2, 0)),
        jnp.transpose(slot_ids, (1, 2, 0)),
        jnp.transpose(route_probs, (1, 2, 0)),
        weights_in,
        weights_out,
    )
    gtok, gprob, gin, gout = pl.pallas_call(
        copy_kernel,
        out_shape=tuple(jax.ShapeDtypeStruct(a.shape, a.dtype) for a in (gtok, gprob, gin, gout)),
        in_specs=[vmem] * 4,
        out_specs=(anywhere,) * 4,
        scratch_shapes=[dma((4,))],
        name="results",
    )(*(pltpu.with_memory_space_constraint(a, pltpu.VMEM) for a in (gtok, gprob, gin, gout)))
    return gtok, jnp.transpose(gprob, (2, 0, 1)), gin, gout


def solution(mesh):
    return jax.shard_map(
        body,
        mesh=mesh,
        in_specs=(
            P(("dp", "expert"), None),
            P(("dp", "expert"), None),
            P(("dp", "expert"), None, None),
            P(("dp", "expert"), None, None),
            P(("dp", "expert"), None, None),
            P("expert", None, "dp", None),
            P("expert", "dp", None),
        ),
        out_specs=(
            P(("dp", "expert"), None),
            P(("dp", "expert"), None, None),
            P("expert", None, "dp", None),
            P("expert", "dp", None),
        ),
        check_vma=False,
    )
```

```python
import functools

import jax
import jax.numpy as jnp
from jax import lax
from jax.experimental import pallas as pl
from jax.experimental.pallas import tpu as pltpu
from jax.sharding import PartitionSpec as P

H = 8
NX = 4
NH = 2
MESH = pl.DeviceIdType.MESH
F32 = jnp.float32
BF16 = jnp.bfloat16
BLOCKS = 4
FLIP = True
GRID = {16: (4, 2, 2), 2: (1, 1, 2)}


def dot_nn(a, b):
    return lax.dot_general(a, b, (((1,), (0,)), ((), ())), preferred_element_type=F32)


def dot_nt(a, b):
    return lax.dot_general(a, b, (((1,), (1,)), ((), ())), preferred_element_type=F32)


def dot_tn(a, b):
    return lax.dot_general(a, b, (((0,), (0,)), ((), ())), preferred_element_type=F32)


def send_order(nz, ny, nc):
    order = []
    for dc in range(nc):
        for s in range(nz):
            for dy in range(ny):
                order.append((dy, (3 * dy + s) % nz, dc))
    return order


def kernel(
    dims,
    tok,
    cot,
    ids_in,
    slots_in,
    probs_in,
    w_in,
    w_out,
    gtok,
    gprob,
    gin,
    gout,
    ids_buf,
    slots_buf,
    probs_buf,
    place_row,
    prob_row,
    far_acc,
    rows_buf,
    xs_send,
    xs_all,
    wall,
    acts,
    dx,
    racc,
    rs_far,
    rs_sum,
    rs_dir,
    back,
    r_send,
    r_back,
    w_ssem,
    w_rsem,
    x_ssem,
    x_rsem,
    g_ssem,
    g_rsem,
    d_ssem,
    d_rsem,
    r_ssem,
    r_rsem,
    l_sem,
):
    ng, toks, d, fs, cap = dims
    nz, nyl, nc = GRID[ng]
    ny = NH * nyl
    peers = NH * ng
    rows = toks * H
    slots = peers * cap
    half = fs // 2
    fc = NH * fs
    jb = slots // BLOCKS
    per = peers // BLOCKS
    order = send_order(nz, ny, nc)

    dp = lax.axis_index("dp")
    g = lax.axis_index("expert")
    x = dp // NH
    h = dp % NH
    core = g % nc
    y = h * nyl + (g // nc) % nyl
    z = g // (nc * nyl)
    right = (x + 1) % NX
    left = (x + 3) % NX
    far = (x + 2) % NX
    other = 1 - h
    me = g * NH + h

    def place_of(ty, tz, tc):
        return ((tz * nyl + ty % nyl) * nc + tc) * NH + ty // nyl

    def target(t):
        dy, dz, dc = order[t]
        sign = 1 - 2 * core if FLIP else 1
        return place_of(
            (y + sign * dy + ny) % ny, (z + sign * dz + nz) % nz, (core + dc) % nc
        )

    def source(t):
        dy, dz, dc = order[t]
        tc = (core + dc) % nc
        sign = 1 - 2 * tc if FLIP else 1
        return place_of((y - sign * dy + ny) % ny, (z - sign * dz + nz) % nz, tc)

    def device(u):
        return (x * NH + u % NH, u // NH)

    def remote(src, dst, ssem, rsem, to):
        return pltpu.make_async_remote_copy(
            src_ref=src,
            dst_ref=dst,
            send_sem=ssem,
            recv_sem=rsem,
            device_id=to,
            device_id_type=MESH,
        )

    barrier = pltpu.get_barrier_semaphore()
    to_right = (right * NH + h, g)
    to_left = (left * NH + h, g)
    to_partner = (x * NH + other, g)
    for t in range(1, peers):
        pl.semaphore_signal(barrier, inc=1, device_id=device(target(t)), device_id_type=MESH)
    for to in (to_right, to_left):
        pl.semaphore_signal(barrier, inc=1, device_id=to, device_id_type=MESH)

    local = []
    for k, src in enumerate((tok, cot)):
        for n in range(H):
            dst = rows_buf.at[pl.ds((k * H + n) * toks, toks)]
            local.append((src.at[:, pl.ds(n * d, d)], dst))
    local.append((w_in.at[h], wall.at[x, pl.ds(0, 2), h]))
    local.append((w_out.at[h], wall.at[x, 2, h]))
    local = [pltpu.make_async_copy(a, b, l_sem.at[n]) for n, (a, b) in enumerate(local)]
    for c in local:
        c.start()
    routes = ((ids_in, ids_buf), (slots_in, slots_buf), (probs_in, probs_buf))
    routes = [
        pltpu.make_async_copy(a, b, l_sem.at[2 * H + 2 + n]) for n, (a, b) in enumerate(routes)
    ]
    for c in routes:
        c.start()
    pl.semaphore_wait(barrier, peers + 1)

    def wcopy(k, src, dst, to):
        return remote(src, dst, w_ssem.at[k], w_rsem.at[k], to)

    first = [
        wcopy(0, w_in.at[other], wall.at[x, pl.ds(0, 2), h], to_partner),
        wcopy(1, w_out.at[other], wall.at[x, 2, h], to_partner),
        wcopy(2, w_in.at[h], wall.at[x, pl.ds(0, 2), h], to_right),
        wcopy(3, w_out.at[h], wall.at[x, 2, h], to_right),
        wcopy(4, w_in.at[h], wall.at[x, pl.ds(0, 2), h], to_left),
        wcopy(5, w_out.at[h], wall.at[x, 2, h], to_left),
    ]
    for c in first:
        c.start()

    for c in routes:
        c.wait()
    place = ids_buf[...] * cap + slots_buf[...]
    probs = probs_buf[...].astype(F32)
    for k in range(2):
        place_row[k : k + 1, :] = jnp.concatenate([place[n, k : k + 1] for n in range(H)], axis=1)
        prob_row[k : k + 1, :] = jnp.concatenate([probs[n, k : k + 1] for n in range(H)], axis=1)
    for c in local:
        c.wait()

    pairs = nz * nyl
    width = min(2, pairs)
    span = NH * cap

    def xs_copy(t):
        u = target(t)
        return remote(xs_send.at[u], xs_all.at[t], x_ssem.at[t], x_rsem.at[t], device(u))

    for dc in range(nc):
        cc = (core + dc) % nc

        def dispatch(i, carry):
            row = lax.broadcasted_iota(jnp.int32, (width * span, rows), 0)
            ids = row + ((i * width * nc + cc) * span)
            if width == 2:
                ids = ids + jnp.where(row >= span, (nc - 1) * span, 0)
            hit0 = place_row[0:1, :] == ids
            hit1 = place_row[1:2, :] == ids
            one = jnp.where(hit0 | hit1, 1.0, 0.0).astype(BF16)
            wgt = jnp.where(hit0, prob_row[0:1, :], jnp.where(hit1, prob_row[1:2, :], 0.0))
            xr = dot_nn(one, rows_buf[0:rows, :]).astype(BF16)
            sr = dot_nn(wgt.astype(BF16), rows_buf[rows : 2 * rows, :]).astype(BF16)
            for j in range(width):
                e0 = ((i * width + j) * nc + cc) * NH
                for k in range(NH):
                    at = (j * NH + k) * cap
                    xs_send[e0 + k, 0] = xr[at : at + cap, :]
                    xs_send[e0 + k, 1] = sr[at : at + cap, :]
            return carry

        lax.fori_loop(0, pairs // width, dispatch, 0)
        for t in range(1, peers):
            if order[t][2] == dc:
                xs_copy(t).start()

    xs_all[0] = xs_send[me]
    racc[...] = jnp.zeros_like(racc)
    dx[...] = jnp.zeros_like(dx)

    def wforward(k, slot, part_rows, plane, to):
        ref = wall.at[slot, pl.ds(0, 3), plane, part_rows]
        return wcopy(k, ref, ref, to)

    top, bottom, full = pl.ds(0, half), pl.ds(half, half), pl.ds(0, fs)

    def xs_wait(i, share=1):
        count = per // share
        for t in range(max(1, i * count), (i + 1) * count):
            xs_copy(t).wait_recv()

    def block(xc, i, share=1):
        per, jb = peers // BLOCKS // share, slots // BLOCKS // share
        at = pl.ds(pl.multiple_of(i * jb, jb), jb)
        some = pl.ds(i * per, per)
        xb = xs_all[some, 0].reshape(jb, d)
        sb = xs_all[some, 1].reshape(jb, d)
        wg = wall[xc, 0].reshape(fc, d)
        wu = wall[xc, 1].reshape(fc, d)
        wo = wall[xc, 2].reshape(fc, d)
        gate = dot_nt(wg, xb)
        up = dot_nt(wu, xb)
        dh = dot_nt(wo, sb)
        sg = 0.5 * jnp.tanh(0.5 * gate) + 0.5
        a = gate * sg
        du = dh * a
        dg = dh * up * (sg + a * (1.0 - sg))
        dgb = dg.astype(BF16)
        dub = du.astype(BF16)
        acts[xc, 0, :, :, at] = dgb.reshape(NH, fs, jb)
        acts[xc, 1, :, :, at] = dub.reshape(NH, fs, jb)
        acts[xc, 2, :, :, at] = (a * up).astype(BF16).reshape(NH, fs, jb)
        racc[:, at] += jnp.sum((du * up).reshape(fc // 8, 8, jb), axis=0)
        dx[at, :] += dot_tn(dgb, wg) + dot_tn(dub, wu)

    def sweep(count, xc_of, i_of):
        def step(n, carry):
            block(xc_of(n), i_of(n))
            return carry

        lax.fori_loop(0, count, step, 0)

    first[2].wait_recv()
    first[3].wait_recv()
    f6 = wforward(6, left, top, h, to_right)
    f6.start()
    first[4].wait_recv()
    first[5].wait_recv()
    f7 = wforward(7, right, bottom, h, to_left)
    f7.start()
    first[0].wait_recv()
    first[1].wait_recv()
    f8 = wforward(8, x, full, other, to_right)
    f8.start()
    f9 = wforward(9, x, full, other, to_left)
    f9.start()
    xs_wait(0)
    sweep(1, lambda n: x, lambda n: n * 0)
    f8.wait_recv()
    f10 = wforward(10, left, top, other, to_right)
    f10.start()
    f9.wait_recv()
    f11 = wforward(11, right, bottom, other, to_left)
    f11.start()
    sweep(2, lambda n: (x + 1 + 2 * n) % NX, lambda n: n * 0)
    xs_wait(1)
    sweep(3, lambda n: (x + jnp.where(n == 2, 3, n)) % NX, lambda n: n * 0 + 1)
    for c in (f6, f7, f10, f11):
        c.wait_recv()
    sweep(2, lambda n: far, lambda n: n)
    xs_wait(2)
    sweep(4, lambda n: (x + 2 + n) % NX, lambda n: n * 0 + 2)

    share = min(2, per)
    held = peers - per // share
    before = held * cap
    for i in range((BLOCKS - 1) * share, BLOCKS * share - 1):
        xs_wait(i, share)
        block(far, i, share)
    for m in range(3):
        far_acc[m] = dot_nn(
            acts[far, m, :, :, 0:before].reshape(fc, before),
            xs_all[0:held, m // 2].reshape(before, d),
        )
    xs_wait(BLOCKS * share - 1, share)

    def give(i):
        for k in range(per):
            t = i * per + k
            dst = rows_buf.at[pl.ds(t * cap, cap)]
            if t:
                u = source(t)
                remote(dst, back.at[me], d_ssem.at[t], d_rsem.at[me], device(u)).start()
                remote(r_send.at[t], r_back.at[me], r_ssem.at[t], r_rsem.at[me], device(u)).start()
            else:
                back[me] = rows_buf[0:cap, :]
                r_back[me] = r_send[0]

    def finish(i):
        rows_buf[i * jb : (i + 1) * jb, :] = dx[i * jb : (i + 1) * jb, :].astype(BF16)
        r_row = jnp.sum(racc[:, i * jb : (i + 1) * jb], axis=0, keepdims=True)
        for k in range(per):
            v = r_row[:, k * cap : (k + 1) * cap]
            r_send[i * per + k] = jnp.broadcast_to(jnp.concatenate([v, v], axis=1), (8, 128))

    planes = (other, h)

    def gcopy(k, src, dst, to):
        return remote(src, dst, g_ssem.at[k], g_rsem.at[k], to)

    def piece(xc, part_rows, plane):
        return acts.at[xc, pl.ds(0, 3), plane, part_rows, pl.ds(0, d)]

    far_right = [gcopy(p, piece(far, top, planes[p]), rs_far.at[0, p], to_right) for p in (0, 1)]
    far_left = [
        gcopy(2 + p, piece(far, bottom, planes[p]), rs_far.at[1, p], to_left) for p in (0, 1)
    ]
    dir_right = [
        gcopy(4 + p, piece(right, bottom, planes[p]), rs_dir.at[0, p], to_right) for p in (0, 1)
    ]
    dir_left = [
        gcopy(6 + p, piece(left, top, planes[p]), rs_dir.at[1, p], to_left) for p in (0, 1)
    ]
    sum_right = [
        gcopy(8 + p, piece(right, top, planes[p]), rs_sum.at[0, p], to_right) for p in (0, 1)
    ]
    sum_left = [
        gcopy(10 + p, piece(left, bottom, planes[p]), rs_sum.at[1, p], to_left) for p in (0, 1)
    ]

    def weight_grads(xc):
        xa = xs_all[:, 0].reshape(slots, d)
        sa = xs_all[:, 1].reshape(slots, d)
        for m, against in ((0, xa), (1, xa), (2, sa)):
            grad = dot_nn(acts[xc, m].reshape(fc, slots), against)
            acts[xc, m, :, :, 0:d] = grad.astype(BF16).reshape(NH, fs, d)

    def add_far(side, p):
        xc, part_rows = (right, top) if side == 0 else (left, bottom)
        for m in range(3):
            mine = acts[xc, m, planes[p], part_rows, 0:d].astype(F32)
            acts[xc, m, planes[p], part_rows, 0:d] = (
                rs_far[side, p, m].astype(F32) + mine
            ).astype(BF16)

    block(far, BLOCKS * share - 1, share)
    for m in range(3):
        grad = far_acc[m] + dot_nn(
            acts[far, m, :, :, before:slots].reshape(fc, slots - before),
            xs_all[held:peers, m // 2].reshape(slots - before, d),
        )
        acts[far, m, :, :, 0:d] = grad.astype(BF16).reshape(NH, fs, d)
    for p in (0, 1):
        far_right[p].start()
        far_left[p].start()
    for i in range(BLOCKS - 1):
        finish(i)
        give(i)

    def last(n, carry):
        xc = (x + jnp.where(n == 0, 1, jnp.where(n == 1, 3, 0))) % NX
        block(xc, BLOCKS - 1)

        @pl.when(n == 2)
        def _():
            finish(BLOCKS - 1)
            give(BLOCKS - 1)

        weight_grads(xc)

        @pl.when(n == 0)
        def _():
            dir_right[0].start()

        @pl.when(n == 1)
        def _():
            dir_left[0].start()
            far_right[0].wait_recv()
            add_far(0, 0)
            sum_right[0].start()
            dir_right[1].start()
            far_left[0].wait_recv()
            add_far(1, 0)
            sum_left[0].start()
            dir_left[1].start()

        return carry

    lax.fori_loop(0, NX - 1, last, 0)
    far_right[1].wait_recv()
    add_far(0, 1)
    sum_right[1].start()
    far_left[1].wait_recv()
    add_far(1, 1)
    sum_left[1].start()

    def total(m, p, lower):
        mine = acts[x, m, planes[p], pl.ds(half if lower else 0, half), 0:d].astype(F32)
        if lower:
            got = rs_dir[0, p, m].astype(F32) + rs_sum[1, p, m].astype(F32)
        else:
            got = rs_dir[1, p, m].astype(F32) + rs_sum[0, p, m].astype(F32)
        return (mine + got).astype(BF16)

    for c in (dir_right, dir_left, sum_right, sum_left):
        c[0].wait_recv()
    for m in range(3):
        acts[x, m, other, 0:half, 0:d] = total(m, 0, False)
        acts[x, m, other, half:fs, 0:d] = total(m, 0, True)
    swap_in = gcopy(12, acts.at[x, pl.ds(0, 2), other, full, pl.ds(0, d)], gin.at[h], to_partner)
    swap_out = gcopy(13, acts.at[x, 2, other, full, pl.ds(0, d)], gout.at[h], to_partner)
    swap_in.start()
    swap_out.start()

    for t in range(1, peers):
        u = target(t)
        dst = rows_buf.at[pl.ds(0, cap)]
        remote(dst, back.at[u], d_ssem.at[t], d_rsem.at[u], device(u)).wait_recv()
        remote(r_send.at[0], r_back.at[u], r_ssem.at[t], r_rsem.at[u], device(u)).wait_recv()
    flat = jnp.concatenate(
        [place_row[k : k + 1, n * toks : (n + 1) * toks] for n in range(H) for k in range(2)],
        axis=0,
    )
    cols = jnp.transpose(flat.astype(F32), (1, 0)).astype(jnp.int32)
    ids = lax.broadcasted_iota(jnp.int32, (toks, slots), 1)
    for n in range(H):
        hit = (cols[:, 2 * n : 2 * n + 1] == ids) | (cols[:, 2 * n + 1 : 2 * n + 2] == ids)
        one = jnp.where(hit, 1.0, 0.0).astype(BF16)
        grad = dot_nn(one, back[...].reshape(slots, d))
        gtok[:, n * d : (n + 1) * d] = grad.astype(BF16)

    r_mine = r_back[:, 0, :]
    for k in range(2):
        pr = place_row[k : k + 1, :]
        expert = lax.shift_right_logical(pr, cap.bit_length() - 1)
        slot = lax.bitwise_and(pr, cap - 1)
        pick = jnp.where(lax.broadcasted_iota(jnp.int32, (peers, rows), 0) == expert, 1.0, 0.0)
        table = lax.dot_general(
            r_mine,
            pick,
            (((0,), (0,)), ((), ())),
            precision=lax.Precision.HIGHEST,
            preferred_element_type=F32,
        )
        lanes = lax.broadcasted_iota(jnp.int32, (128, rows), 0)
        value = jnp.sum(jnp.where(lanes == slot, table, 0.0), axis=0, keepdims=True)
        ratio = value / prob_row[k : k + 1, :]
        for n in range(H):
            gprob[n, k : k + 1, :] = ratio[:, n * toks : (n + 1) * toks]


    for c in (dir_right, dir_left, sum_right, sum_left):
        c[1].wait_recv()
    for m in range(2):
        gin[h, m, 0:half] = total(m, 1, False)
        gin[h, m, half:fs] = total(m, 1, True)
    gout[h, 0:half] = total(2, 1, False)
    gout[h, half:fs] = total(2, 1, True)

    for c in first + [f6, f7, f8, f9, f10, f11]:
        c.wait_send()
    for c in (far_right, far_left, dir_right, dir_left, sum_right, sum_left):
        c[0].wait_send()
        c[1].wait_send()
    for t in range(1, peers):
        xs_copy(t).wait_send()
        dst = rows_buf.at[pl.ds(0, cap)]
        remote(dst, back.at[0], d_ssem.at[t], d_rsem.at[0], device(source(t))).wait_send()
        remote(r_send.at[0], r_back.at[0], r_ssem.at[t], r_rsem.at[0], device(source(t))).wait_send()
    swap_in.wait()
    swap_out.wait()


def copy_kernel(*refs):
    ins, outs, sem = refs[0:4], refs[4:8], refs[8]
    moves = [pltpu.make_async_copy(ins[n], outs[n], sem.at[n]) for n in range(4)]
    for c in moves:
        c.start()
    for c in moves:
        c.wait()


def body(tokens, cotangent, expert_ids, slot_ids, route_probs, weights_in, weights_out):
    ng = lax.axis_size("expert")
    toks = tokens.shape[0]
    d = tokens.shape[1] // H
    fs = weights_in.shape[2]
    peers = NH * ng
    rows = toks * H
    cap = rows * 2 // peers
    slots = peers * cap
    half = fs // 2
    fc = NH * fs

    vmem = pl.BlockSpec(memory_space=pltpu.VMEM)
    anywhere = pl.BlockSpec(memory_space=pl.ANY)
    dma = pltpu.SemaphoreType.DMA
    gtok, gprob, gin, gout = pl.pallas_call(
        functools.partial(kernel, (ng, toks, d, fs, cap)),
        out_shape=(
            pltpu.VMEM((toks, H * d), BF16),
            pltpu.VMEM((H, 2, toks), F32),
            pltpu.VMEM((2, 2, fs, d), BF16),
            pltpu.VMEM((2, fs, d), BF16),
        ),
        in_specs=[anywhere] * 7,
        out_specs=(vmem,) * 4,
        scratch_shapes=[
            pltpu.VMEM((H, 2, toks), jnp.int32),
            pltpu.VMEM((H, 2, toks), jnp.int32),
            pltpu.VMEM((H, 2, toks), BF16),
            pltpu.VMEM((2, rows), jnp.int32),
            pltpu.VMEM((2, rows), F32),
            pltpu.VMEM((3, fc, d), F32),
            pltpu.VMEM((2 * rows, d), BF16),
            pltpu.VMEM((peers, 2, cap, d), BF16),
            pltpu.VMEM((peers, 2, cap, d), BF16),
            pltpu.VMEM((NX, 3, NH, fs, d), BF16),
            pltpu.VMEM((NX, 3, NH, fs, slots), BF16),
            pltpu.VMEM((slots, d), F32),
            pltpu.VMEM((8, slots), F32),
            pltpu.VMEM((2, 2, 3, half, d), BF16),
            pltpu.VMEM((2, 2, 3, half, d), BF16),
            pltpu.VMEM((2, 2, 3, half, d), BF16),
            pltpu.VMEM((peers, cap, d), BF16),
            pltpu.VMEM((peers, 8, 128), F32),
            pltpu.VMEM((peers, 8, 128), F32),
            dma((12,)),
            dma((12,)),
            dma((peers,)),
            dma((peers,)),
            dma((14,)),
            dma((14,)),
            dma((peers,)),
            dma((peers,)),
            dma((peers,)),
            dma((peers,)),
            dma((2 * H + 2 + 3,)),
        ],
        compiler_params=pltpu.CompilerParams(
            collective_id=0, has_side_effects=True, vmem_limit_bytes=60_000_000
        ),
        name="moe_backward",
    )(
        tokens,
        cotangent,
        jnp.transpose(expert_ids, (1, 2, 0)),
        jnp.transpose(slot_ids, (1, 2, 0)),
        jnp.transpose(route_probs, (1, 2, 0)),
        weights_in,
        weights_out,
    )
    gtok, gprob, gin, gout = pl.pallas_call(
        copy_kernel,
        out_shape=tuple(jax.ShapeDtypeStruct(a.shape, a.dtype) for a in (gtok, gprob, gin, gout)),
        in_specs=[vmem] * 4,
        out_specs=(anywhere,) * 4,
        scratch_shapes=[dma((4,))],
        name="results",
    )(*(pltpu.with_memory_space_constraint(a, pltpu.VMEM) for a in (gtok, gprob, gin, gout)))
    return gtok, jnp.transpose(gprob, (2, 0, 1)), gin, gout


def solution(mesh):
    return jax.shard_map(
        body,
        mesh=mesh,
        in_specs=(
            P(("dp", "expert"), None),
            P(("dp", "expert"), None),
            P(("dp", "expert"), None, None),
            P(("dp", "expert"), None, None),
            P(("dp", "expert"), None, None),
            P("expert", None, "dp", None),
            P("expert", "dp", None),
        ),
        out_specs=(
            P(("dp", "expert"), None),
            P(("dp", "expert"), None, None),
            P("expert", None, "dp", None),
            P("expert", "dp", None),
        ),
        check_vma=False,
    )
```

```python
import functools

import jax
import jax.numpy as jnp
from jax import lax
from jax.experimental import pallas as pl
from jax.experimental.pallas import tpu as pltpu
from jax.sharding import PartitionSpec as P

H = 8
NX = 4
NH = 2
MESH = pl.DeviceIdType.MESH
F32 = jnp.float32
BF16 = jnp.bfloat16
BLOCKS = 4
FLIP = True
GRID = {16: (4, 2, 2), 2: (1, 1, 2)}


def dot_nn(a, b):
    return lax.dot_general(a, b, (((1,), (0,)), ((), ())), preferred_element_type=F32)


def dot_nt(a, b):
    return lax.dot_general(a, b, (((1,), (1,)), ((), ())), preferred_element_type=F32)


def dot_tn(a, b):
    return lax.dot_general(a, b, (((0,), (0,)), ((), ())), preferred_element_type=F32)


def send_order(nz, ny, nc):
    order = []
    for dc in range(nc):
        for s in range(nz):
            for dy in range(ny):
                order.append((dy, (3 * dy + s) % nz, dc))
    return order


def kernel(
    dims,
    tok,
    cot,
    ids_in,
    slots_in,
    probs_in,
    w_in,
    w_out,
    gtok,
    gprob,
    gin,
    gout,
    ids_buf,
    slots_buf,
    probs_buf,
    place_row,
    prob_row,
    far_acc,
    rows_buf,
    xs_send,
    xs_all,
    wall,
    acts,
    dx,
    racc,
    rs_far,
    rs_sum,
    rs_dir,
    back,
    r_send,
    r_back,
    w_ssem,
    w_rsem,
    x_ssem,
    x_rsem,
    g_ssem,
    g_rsem,
    d_ssem,
    d_rsem,
    r_ssem,
    r_rsem,
    l_sem,
):
    ng, toks, d, fs, cap = dims
    nz, nyl, nc = GRID[ng]
    ny = NH * nyl
    peers = NH * ng
    rows = toks * H
    slots = peers * cap
    half = fs // 2
    fc = NH * fs
    jb = slots // BLOCKS
    per = peers // BLOCKS
    order = send_order(nz, ny, nc)

    dp = lax.axis_index("dp")
    g = lax.axis_index("expert")
    x = dp // NH
    h = dp % NH
    core = g % nc
    y = h * nyl + (g // nc) % nyl
    z = g // (nc * nyl)
    right = (x + 1) % NX
    left = (x + 3) % NX
    far = (x + 2) % NX
    other = 1 - h
    me = g * NH + h

    def place_of(ty, tz, tc):
        return ((tz * nyl + ty % nyl) * nc + tc) * NH + ty // nyl

    def target(t):
        dy, dz, dc = order[t]
        sign = 1 - 2 * core if FLIP else 1
        return place_of(
            (y + sign * dy + ny) % ny, (z + sign * dz + nz) % nz, (core + dc) % nc
        )

    def source(t):
        dy, dz, dc = order[t]
        tc = (core + dc) % nc
        sign = 1 - 2 * tc if FLIP else 1
        return place_of((y - sign * dy + ny) % ny, (z - sign * dz + nz) % nz, tc)

    def device(u):
        return (x * NH + u % NH, u // NH)

    def remote(src, dst, ssem, rsem, to):
        return pltpu.make_async_remote_copy(
            src_ref=src,
            dst_ref=dst,
            send_sem=ssem,
            recv_sem=rsem,
            device_id=to,
            device_id_type=MESH,
        )

    barrier = pltpu.get_barrier_semaphore()
    to_right = (right * NH + h, g)
    to_left = (left * NH + h, g)
    to_partner = (x * NH + other, g)
    for t in range(1, peers):
        pl.semaphore_signal(barrier, inc=1, device_id=device(target(t)), device_id_type=MESH)
    for to in (to_right, to_left):
        pl.semaphore_signal(barrier, inc=1, device_id=to, device_id_type=MESH)

    local = []
    for k, src in enumerate((tok, cot)):
        for n in range(H):
            dst = rows_buf.at[pl.ds((k * H + n) * toks, toks)]
            local.append((src.at[:, pl.ds(n * d, d)], dst))
    local.append((w_in.at[h], wall.at[x, pl.ds(0, 2), h]))
    local.append((w_out.at[h], wall.at[x, 2, h]))
    local = [pltpu.make_async_copy(a, b, l_sem.at[n]) for n, (a, b) in enumerate(local)]
    for c in local:
        c.start()
    routes = ((ids_in, ids_buf), (slots_in, slots_buf), (probs_in, probs_buf))
    routes = [
        pltpu.make_async_copy(a, b, l_sem.at[2 * H + 2 + n]) for n, (a, b) in enumerate(routes)
    ]
    for c in routes:
        c.start()
    pl.semaphore_wait(barrier, peers + 1)

    def wcopy(k, src, dst, to):
        return remote(src, dst, w_ssem.at[k], w_rsem.at[k], to)

    first = [
        wcopy(0, w_in.at[other], wall.at[x, pl.ds(0, 2), h], to_partner),
        wcopy(1, w_out.at[other], wall.at[x, 2, h], to_partner),
        wcopy(2, w_in.at[h], wall.at[x, pl.ds(0, 2), h], to_right),
        wcopy(3, w_out.at[h], wall.at[x, 2, h], to_right),
        wcopy(4, w_in.at[h], wall.at[x, pl.ds(0, 2), h], to_left),
        wcopy(5, w_out.at[h], wall.at[x, 2, h], to_left),
    ]
    for c in first:
        c.start()

    for c in routes:
        c.wait()
    place = ids_buf[...] * cap + slots_buf[...]
    probs = probs_buf[...].astype(F32)
    for k in range(2):
        place_row[k : k + 1, :] = jnp.concatenate([place[n, k : k + 1] for n in range(H)], axis=1)
        prob_row[k : k + 1, :] = jnp.concatenate([probs[n, k : k + 1] for n in range(H)], axis=1)
    for c in local:
        c.wait()

    pairs = nz * nyl
    width = min(2, pairs)
    span = NH * cap

    def xs_copy(t):
        u = target(t)
        return remote(xs_send.at[u], xs_all.at[t], x_ssem.at[t], x_rsem.at[t], device(u))

    for dc in range(nc):
        cc = (core + dc) % nc

        def dispatch(i, carry):
            row = lax.broadcasted_iota(jnp.int32, (width * span, rows), 0)
            ids = row + ((i * width * nc + cc) * span)
            if width == 2:
                ids = ids + jnp.where(row >= span, (nc - 1) * span, 0)
            hit0 = place_row[0:1, :] == ids
            hit1 = place_row[1:2, :] == ids
            one = jnp.where(hit0 | hit1, 1.0, 0.0).astype(BF16)
            wgt = jnp.where(hit0, prob_row[0:1, :], jnp.where(hit1, prob_row[1:2, :], 0.0))
            xr = dot_nn(one, rows_buf[0:rows, :]).astype(BF16)
            sr = dot_nn(wgt.astype(BF16), rows_buf[rows : 2 * rows, :]).astype(BF16)
            for j in range(width):
                e0 = ((i * width + j) * nc + cc) * NH
                for k in range(NH):
                    at = (j * NH + k) * cap
                    xs_send[e0 + k, 0] = xr[at : at + cap, :]
                    xs_send[e0 + k, 1] = sr[at : at + cap, :]
            return carry

        lax.fori_loop(0, pairs // width, dispatch, 0)
        for t in range(1, peers):
            if order[t][2] == dc:
                xs_copy(t).start()

    xs_all[0] = xs_send[me]
    racc[...] = jnp.zeros_like(racc)
    dx[...] = jnp.zeros_like(dx)

    def wforward(k, slot, part_rows, plane, to):
        ref = wall.at[slot, pl.ds(0, 3), plane, part_rows]
        return wcopy(k, ref, ref, to)

    top, bottom, full = pl.ds(0, half), pl.ds(half, half), pl.ds(0, fs)

    def xs_wait(i, share=1):
        count = per // share
        for t in range(max(1, i * count), (i + 1) * count):
            xs_copy(t).wait_recv()

    def block(xc, i, share=1):
        per, jb = peers // BLOCKS // share, slots // BLOCKS // share
        at = pl.ds(pl.multiple_of(i * jb, jb), jb)
        some = pl.ds(i * per, per)
        xb = xs_all[some, 0].reshape(jb, d)
        sb = xs_all[some, 1].reshape(jb, d)
        wg = wall[xc, 0].reshape(fc, d)
        wu = wall[xc, 1].reshape(fc, d)
        wo = wall[xc, 2].reshape(fc, d)
        gate = dot_nt(wg, xb)
        up = dot_nt(wu, xb)
        dh = dot_nt(wo, sb)
        sg = 1.0 / (1.0 + jnp.exp(-gate))
        a = gate * sg
        du = dh * a
        dg = dh * up * (sg + a * (1.0 - sg))
        dgb = dg.astype(BF16)
        dub = du.astype(BF16)
        acts[xc, 0, :, :, at] = dgb.reshape(NH, fs, jb)
        acts[xc, 1, :, :, at] = dub.reshape(NH, fs, jb)
        acts[xc, 2, :, :, at] = (a * up).astype(BF16).reshape(NH, fs, jb)
        racc[:, at] += jnp.sum((du * up).reshape(fc // 8, 8, jb), axis=0)
        dx[at, :] += dot_tn(dgb, wg) + dot_tn(dub, wu)

    def sweep(count, xc_of, i_of):
        def step(n, carry):
            block(xc_of(n), i_of(n))
            return carry

        lax.fori_loop(0, count, step, 0)

    first[2].wait_recv()
    first[3].wait_recv()
    f6 = wforward(6, left, top, h, to_right)
    f6.start()
    first[4].wait_recv()
    first[5].wait_recv()
    f7 = wforward(7, right, bottom, h, to_left)
    f7.start()
    first[0].wait_recv()
    first[1].wait_recv()
    f8 = wforward(8, x, full, other, to_right)
    f8.start()
    f9 = wforward(9, x, full, other, to_left)
    f9.start()
    xs_wait(0)
    sweep(1, lambda n: x, lambda n: n * 0)
    f8.wait_recv()
    f10 = wforward(10, left, top, other, to_right)
    f10.start()
    f9.wait_recv()
    f11 = wforward(11, right, bottom, other, to_left)
    f11.start()
    sweep(2, lambda n: (x + 1 + 2 * n) % NX, lambda n: n * 0)
    xs_wait(1)
    sweep(3, lambda n: (x + jnp.where(n == 2, 3, n)) % NX, lambda n: n * 0 + 1)
    for c in (f6, f7, f10, f11):
        c.wait_recv()
    sweep(2, lambda n: far, lambda n: n)
    xs_wait(2)
    sweep(4, lambda n: (x + 2 + n) % NX, lambda n: n * 0 + 2)

    share = min(2, per)
    held = peers - per // share
    before = held * cap
    for i in range((BLOCKS - 1) * share, BLOCKS * share - 1):
        xs_wait(i, share)
        block(far, i, share)
    for m in range(3):
        far_acc[m] = dot_nn(
            acts[far, m, :, :, 0:before].reshape(fc, before),
            xs_all[0:held, m // 2].reshape(before, d),
        )
    xs_wait(BLOCKS * share - 1, share)

    def give(i):
        for k in range(per):
            t = i * per + k
            dst = rows_buf.at[pl.ds(t * cap, cap)]
            if t:
                u = source(t)
                remote(dst, back.at[me], d_ssem.at[t], d_rsem.at[me], device(u)).start()
                remote(r_send.at[t], r_back.at[me], r_ssem.at[t], r_rsem.at[me], device(u)).start()
            else:
                back[me] = rows_buf[0:cap, :]
                r_back[me] = r_send[0]

    def finish(i):
        rows_buf[i * jb : (i + 1) * jb, :] = dx[i * jb : (i + 1) * jb, :].astype(BF16)
        r_row = jnp.sum(racc[:, i * jb : (i + 1) * jb], axis=0, keepdims=True)
        for k in range(per):
            v = r_row[:, k * cap : (k + 1) * cap]
            r_send[i * per + k] = jnp.broadcast_to(jnp.concatenate([v, v], axis=1), (8, 128))

    planes = (other, h)

    def gcopy(k, src, dst, to):
        return remote(src, dst, g_ssem.at[k], g_rsem.at[k], to)

    def piece(xc, part_rows, plane):
        return acts.at[xc, pl.ds(0, 3), plane, part_rows, pl.ds(0, d)]

    far_right = [gcopy(p, piece(far, top, planes[p]), rs_far.at[0, p], to_right) for p in (0, 1)]
    far_left = [
        gcopy(2 + p, piece(far, bottom, planes[p]), rs_far.at[1, p], to_left) for p in (0, 1)
    ]
    dir_right = [
        gcopy(4 + p, piece(right, bottom, planes[p]), rs_dir.at[0, p], to_right) for p in (0, 1)
    ]
    dir_left = [
        gcopy(6 + p, piece(left, top, planes[p]), rs_dir.at[1, p], to_left) for p in (0, 1)
    ]
    sum_right = [
        gcopy(8 + p, piece(right, top, planes[p]), rs_sum.at[0, p], to_right) for p in (0, 1)
    ]
    sum_left = [
        gcopy(10 + p, piece(left, bottom, planes[p]), rs_sum.at[1, p], to_left) for p in (0, 1)
    ]

    def weight_grads(xc):
        xa = xs_all[:, 0].reshape(slots, d)
        sa = xs_all[:, 1].reshape(slots, d)
        for m, against in ((0, xa), (1, xa), (2, sa)):
            grad = dot_nn(acts[xc, m].reshape(fc, slots), against)
            acts[xc, m, :, :, 0:d] = grad.astype(BF16).reshape(NH, fs, d)

    def add_far(side, p):
        xc, part_rows = (right, top) if side == 0 else (left, bottom)
        for m in range(3):
            mine = acts[xc, m, planes[p], part_rows, 0:d].astype(F32)
            acts[xc, m, planes[p], part_rows, 0:d] = (
                rs_far[side, p, m].astype(F32) + mine
            ).astype(BF16)

    block(far, BLOCKS * share - 1, share)
    for m in range(3):
        grad = far_acc[m] + dot_nn(
            acts[far, m, :, :, before:slots].reshape(fc, slots - before),
            xs_all[held:peers, m // 2].reshape(slots - before, d),
        )
        acts[far, m, :, :, 0:d] = grad.astype(BF16).reshape(NH, fs, d)
    for p in (0, 1):
        far_right[p].start()
        far_left[p].start()
    for i in range(BLOCKS - 1):
        finish(i)
        give(i)

    def last(n, carry):
        xc = (x + jnp.where(n == 0, 1, jnp.where(n == 1, 3, 0))) % NX
        block(xc, BLOCKS - 1)

        @pl.when(n == 2)
        def _():
            finish(BLOCKS - 1)
            give(BLOCKS - 1)

        weight_grads(xc)

        @pl.when(n == 0)
        def _():
            dir_right[0].start()

        @pl.when(n == 1)
        def _():
            dir_left[0].start()
            far_right[0].wait_recv()
            add_far(0, 0)
            sum_right[0].start()
            dir_right[1].start()
            far_left[0].wait_recv()
            add_far(1, 0)
            sum_left[0].start()
            dir_left[1].start()

        return carry

    lax.fori_loop(0, NX - 1, last, 0)
    far_right[1].wait_recv()
    add_far(0, 1)
    sum_right[1].start()
    far_left[1].wait_recv()
    add_far(1, 1)
    sum_left[1].start()

    def total(m, p, lower):
        mine = acts[x, m, planes[p], pl.ds(half if lower else 0, half), 0:d].astype(F32)
        if lower:
            got = rs_dir[0, p, m].astype(F32) + rs_sum[1, p, m].astype(F32)
        else:
            got = rs_dir[1, p, m].astype(F32) + rs_sum[0, p, m].astype(F32)
        return (mine + got).astype(BF16)

    for c in (dir_right, dir_left, sum_right, sum_left):
        c[0].wait_recv()
    for m in range(3):
        acts[x, m, other, 0:half, 0:d] = total(m, 0, False)
        acts[x, m, other, half:fs, 0:d] = total(m, 0, True)
    swap_in = gcopy(12, acts.at[x, pl.ds(0, 2), other, full, pl.ds(0, d)], gin.at[h], to_partner)
    swap_out = gcopy(13, acts.at[x, 2, other, full, pl.ds(0, d)], gout.at[h], to_partner)
    swap_in.start()
    swap_out.start()

    for t in range(1, peers):
        u = target(t)
        dst = rows_buf.at[pl.ds(0, cap)]
        remote(dst, back.at[u], d_ssem.at[t], d_rsem.at[u], device(u)).wait_recv()
        remote(r_send.at[0], r_back.at[u], r_ssem.at[t], r_rsem.at[u], device(u)).wait_recv()
    flat = jnp.concatenate(
        [place_row[k : k + 1, n * toks : (n + 1) * toks] for n in range(H) for k in range(2)],
        axis=0,
    )
    cols = jnp.transpose(flat.astype(F32), (1, 0)).astype(jnp.int32)
    ids = lax.broadcasted_iota(jnp.int32, (toks, slots), 1)
    for n in range(H):
        hit = (cols[:, 2 * n : 2 * n + 1] == ids) | (cols[:, 2 * n + 1 : 2 * n + 2] == ids)
        one = jnp.where(hit, 1.0, 0.0).astype(BF16)
        grad = dot_nn(one, back[...].reshape(slots, d))
        gtok[:, n * d : (n + 1) * d] = grad.astype(BF16)

    r_mine = r_back[:, 0, :]
    for k in range(2):
        pr = place_row[k : k + 1, :]
        expert = lax.shift_right_logical(pr, cap.bit_length() - 1)
        slot = lax.bitwise_and(pr, cap - 1)
        pick = jnp.where(lax.broadcasted_iota(jnp.int32, (peers, rows), 0) == expert, 1.0, 0.0)
        table = lax.dot_general(
            r_mine,
            pick,
            (((0,), (0,)), ((), ())),
            precision=lax.Precision.HIGHEST,
            preferred_element_type=F32,
        )
        lanes = lax.broadcasted_iota(jnp.int32, (128, rows), 0)
        value = jnp.sum(jnp.where(lanes == slot, table, 0.0), axis=0, keepdims=True)
        ratio = value / prob_row[k : k + 1, :]
        for n in range(H):
            gprob[n, k : k + 1, :] = ratio[:, n * toks : (n + 1) * toks]


    for c in (dir_right, dir_left, sum_right, sum_left):
        c[1].wait_recv()
    for m in range(2):
        gin[h, m, 0:half] = total(m, 1, False)
        gin[h, m, half:fs] = total(m, 1, True)
    gout[h, 0:half] = total(2, 1, False)
    gout[h, half:fs] = total(2, 1, True)

    for c in first + [f6, f7, f8, f9, f10, f11]:
        c.wait_send()
    for c in (far_right, far_left, dir_right, dir_left, sum_right, sum_left):
        c[0].wait_send()
        c[1].wait_send()
    for t in range(1, peers):
        xs_copy(t).wait_send()
        dst = rows_buf.at[pl.ds(0, cap)]
        remote(dst, back.at[0], d_ssem.at[t], d_rsem.at[0], device(source(t))).wait_send()
        remote(r_send.at[0], r_back.at[0], r_ssem.at[t], r_rsem.at[0], device(source(t))).wait_send()
    swap_in.wait()
    swap_out.wait()


def copy_kernel(*refs):
    ins, outs, sem = refs[0:4], refs[4:8], refs[8]
    moves = [pltpu.make_async_copy(ins[n], outs[n], sem.at[n]) for n in range(4)]
    for c in moves:
        c.start()
    for c in moves:
        c.wait()


def body(tokens, cotangent, expert_ids, slot_ids, route_probs, weights_in, weights_out):
    ng = lax.axis_size("expert")
    toks = tokens.shape[0]
    d = tokens.shape[1] // H
    fs = weights_in.shape[2]
    peers = NH * ng
    rows = toks * H
    cap = rows * 2 // peers
    slots = peers * cap
    half = fs // 2
    fc = NH * fs

    vmem = pl.BlockSpec(memory_space=pltpu.VMEM)
    anywhere = pl.BlockSpec(memory_space=pl.ANY)
    dma = pltpu.SemaphoreType.DMA
    gtok, gprob, gin, gout = pl.pallas_call(
        functools.partial(kernel, (ng, toks, d, fs, cap)),
        out_shape=(
            pltpu.VMEM((toks, H * d), BF16),
            pltpu.VMEM((H, 2, toks), F32),
            pltpu.VMEM((2, 2, fs, d), BF16),
            pltpu.VMEM((2, fs, d), BF16),
        ),
        in_specs=[anywhere] * 7,
        out_specs=(vmem,) * 4,
        scratch_shapes=[
            pltpu.VMEM((H, 2, toks), jnp.int32),
            pltpu.VMEM((H, 2, toks), jnp.int32),
            pltpu.VMEM((H, 2, toks), BF16),
            pltpu.VMEM((2, rows), jnp.int32),
            pltpu.VMEM((2, rows), F32),
            pltpu.VMEM((3, fc, d), F32),
            pltpu.VMEM((2 * rows, d), BF16),
            pltpu.VMEM((peers, 2, cap, d), BF16),
            pltpu.VMEM((peers, 2, cap, d), BF16),
            pltpu.VMEM((NX, 3, NH, fs, d), BF16),
            pltpu.VMEM((NX, 3, NH, fs, slots), BF16),
            pltpu.VMEM((slots, d), F32),
            pltpu.VMEM((8, slots), F32),
            pltpu.VMEM((2, 2, 3, half, d), BF16),
            pltpu.VMEM((2, 2, 3, half, d), BF16),
            pltpu.VMEM((2, 2, 3, half, d), BF16),
            pltpu.VMEM((peers, cap, d), BF16),
            pltpu.VMEM((peers, 8, 128), F32),
            pltpu.VMEM((peers, 8, 128), F32),
            dma((12,)),
            dma((12,)),
            dma((peers,)),
            dma((peers,)),
            dma((14,)),
            dma((14,)),
            dma((peers,)),
            dma((peers,)),
            dma((peers,)),
            dma((peers,)),
            dma((2 * H + 2 + 3,)),
        ],
        compiler_params=pltpu.CompilerParams(
            collective_id=0, has_side_effects=True, vmem_limit_bytes=60_000_000
        ),
        name="moe_backward",
    )(
        tokens,
        cotangent,
        jnp.transpose(expert_ids, (1, 2, 0)),
        jnp.transpose(slot_ids, (1, 2, 0)),
        jnp.transpose(route_probs, (1, 2, 0)),
        weights_in,
        weights_out,
    )
    gtok, gprob, gin, gout = pl.pallas_call(
        copy_kernel,
        out_shape=tuple(jax.ShapeDtypeStruct(a.shape, a.dtype) for a in (gtok, gprob, gin, gout)),
        in_specs=[vmem] * 4,
        out_specs=(anywhere,) * 4,
        scratch_shapes=[dma((4,))],
        name="results",
    )(*(pltpu.with_memory_space_constraint(a, pltpu.VMEM) for a in (gtok, gprob, gin, gout)))
    return gtok, jnp.transpose(gprob, (2, 0, 1)), gin, gout


def solution(mesh):
    return jax.shard_map(
        body,
        mesh=mesh,
        in_specs=(
            P(("dp", "expert"), None),
            P(("dp", "expert"), None),
            P(("dp", "expert"), None, None),
            P(("dp", "expert"), None, None),
            P(("dp", "expert"), None, None),
            P("expert", None, "dp", None),
            P("expert", "dp", None),
        ),
        out_specs=(
            P(("dp", "expert"), None),
            P(("dp", "expert"), None, None),
            P("expert", None, "dp", None),
            P("expert", "dp", None),
        ),
        check_vma=False,
    )
```
